32 devices in a mesh: dop: 2 (over core), tm: 16 (over z, y, x).
Axes of the slice: x: 2, y: 2, z: 4, core: 2. Of those that a mesh axis runs over, the one named last changes fastest.
Arguments:
- surveillance: bfloat16 [2, 16, 8192], P(None, 'tm', 'dop'), may hold values from -6 to 6
- reference_signal: bfloat16 [2, 16, 8192], P(None, 'tm', 'dop'), may hold values from -6 to 6
Outputs:
- ambiguity: float32 [2048, 2, 512], P('tm', None, 'dop')
The draws below stay inside these ranges and needn't reach their ends.
All inputs are finite; a program needn't handle non-finite values.
Results may differ from the reference program's by a relative error of at most 0.0029.
Values may be sent and summed in bfloat16 or wider, within the bound.
A program may use at most 128 MiB of HBM per device.

```python
import math
import jax
import jax.numpy as jnp
from jax import lax

F = 512
LAGS = 2048
BLOCK = 8192
BLOCKS = 16
TIME = 131072


def levels(own_key, extent, split, least, high):
    loudness = 1.0
    for axis_at, shards_of in split:
        heights = jax.random.uniform(jax.random.fold_in(jax.random.fold_in(own_key, 6), axis_at), (shards_of,), jnp.float32, least / len(split), high / len(split))
        loudness = loudness * jnp.repeat(jnp.exp(heights), extent[axis_at] // shards_of).reshape((-1,) + (1,) * (len(extent) - 1 - axis_at))
    return loudness


def scatter_about(rng, extent, spread, limit, split=(), held_as=jnp.bfloat16):
    entries = spread * jax.random.normal(rng, extent, jnp.float32)
    if split:
        entries = entries * levels(rng, extent, split, -0.22, 0.18)
    return jnp.clip(entries, -limit, limit).astype(held_as)


def setup_inputs(seed: int = 0) -> dict:
    splits = jax.random.split(jax.random.key(seed), 3)
    return {
        "surveillance": scatter_about(splits[0], (2, BLOCKS, BLOCK), 1.0, 6.0, ((1, 16), (2, 2))),
        "reference_signal": scatter_about(splits[1], (2, BLOCKS, BLOCK), 1.0, 6.0, ((1, 16), (2, 2))),
    }


def toeplitz_rows(segment, height, breadth):
    length = height + breadth - 1
    repeated = jnp.tile(segment, (1, height + 1))[:, :height * (length + 1)]
    return repeated.reshape(2, height, length + 1)[:, :, :breadth]

def mix_rows(samples, sample_index, doppler, window):
    phase_step = jnp.mod(doppler[:, None] * sample_index[None, :], window)
    phase_angle = phase_step.astype(jnp.float32) * (2.0 * math.pi / window)
    cosine = jnp.cos(phase_angle)
    sine_part = jnp.sin(phase_angle)
    real_in = samples[0].astype(jnp.float32)[None, :]
    imag_in = samples[1].astype(jnp.float32)[None, :]
    mixed_real = (real_in * cosine + imag_in * sine_part).astype(jnp.bfloat16)
    mixed_imag = (imag_in * cosine - real_in * sine_part).astype(jnp.bfloat16)
    upper_half = jnp.concatenate([mixed_real, mixed_imag], 1)
    lower_half = jnp.concatenate([mixed_imag, -mixed_real], 1)
    return jnp.concatenate([upper_half, lower_half], 0)

def lag_product(toeplitz, mixed):
    height = toeplitz.shape[1]
    stacked = toeplitz.reshape(2 * height, toeplitz.shape[2])
    return lax.dot_general(stacked, mixed, (((0,), (1,)), ((), ())), preferred_element_type=jnp.float32)

def reference(surveillance, reference_signal):
    signal = surveillance.reshape(2, TIME)
    reference_flat = reference_signal.reshape(2, TIME)
    extended = jnp.concatenate([jnp.zeros((2, LAGS - 1), jnp.bfloat16), reference_flat], 1)
    height = min(512, TIME)
    doppler = jnp.arange(F, dtype=jnp.int32) - F // 2

    def one_step(running, turn_no):
        offset = turn_no * height
        segment = lax.dynamic_slice_in_dim(extended, offset, height + LAGS - 1, 1)[:, ::-1]
        toeplitz = toeplitz_rows(segment, height, LAGS)
        samples = lax.dynamic_slice_in_dim(signal, offset, height, 1)[:, ::-1]
        sample_index = offset + height - 1 - jnp.arange(height, dtype=jnp.int32)
        return (running + lag_product(toeplitz, mix_rows(samples, sample_index, doppler, TIME)), None)
    running, unused = lax.scan(one_step, jnp.zeros((LAGS, 2 * F), jnp.float32), jnp.arange(TIME // height, dtype=jnp.int32))
    return running.reshape(LAGS, 2, F) * (1.0 / math.sqrt(TIME))
```

```python
import functools
import math

import jax
import jax.numpy as jnp
import numpy as np
from jax import lax
from jax.experimental import pallas as pl
from jax.experimental.pallas import tpu as pltpu
from jax.sharding import PartitionSpec as P

F = 512
LAGS = 2048
LANES = 128
SUB = 8
POINTS = 2 * LAGS
N1 = LAGS // LANES
F1 = POINTS // LANES
UNIT = 2 * N1 * 2
MESH = pl.DeviceIdType.MESH


class Plan:
    def __init__(self, times, cuts, window):
        self.times, self.cuts, self.window = times, cuts, window
        self.devices = times * cuts
        self.units = window // (2 * LAGS)
        self.groups = self.units // 4
        self.fine = window // POINTS
        self.shifts = F // self.fine
        self.share = self.devices // self.fine
        self.mine = self.shifts // self.share
        self.per_owner = self.shifts // cuts
        self.owners = self.mine // self.per_owner
        self.lags = LAGS // times


def halves(x):
    high = x.astype(jnp.bfloat16)
    low = (x - high.astype(jnp.float32)).astype(jnp.bfloat16)
    return high, low


def tables(plan):
    a = np.arange(LANES)
    angle = 2.0 * np.pi / LANES * np.mod(a[:, None] * a[None, :], LANES)
    c, s = np.cos(angle), np.sin(angle)
    waves = []
    for sign in (-1.0, 1.0):
        full = np.block([[c, sign * s], [-sign * s, c]])
        high = full.astype(jnp.bfloat16)
        low = (full - high.astype(np.float64)).astype(jnp.bfloat16)
        waves += [high, low]
    turn = 2.0 * np.pi / POINTS * np.arange(F1)[:, None] * a[None, :]
    turns = np.stack([np.cos(turn), -np.sin(turn)], 1)
    sign = np.where(
        (np.arange(F1)[:, None] * np.arange(SUB)[None, :]) % 2 == 1, -1.0, 1.0
    )
    forward = (turns[:, :, None, :] * sign[:, None, :, None]).astype(np.float32)
    scale = 1.0 / (POINTS * math.sqrt(plan.window))
    back = (np.stack([np.cos(turn), np.sin(turn)], 1) * scale).astype(np.float32)
    back = np.broadcast_to(back[:, :, None, :], (F1, 2, SUB, LANES)).copy()
    return np.stack(waves), forward, back


def times_(x, y):
    return x[0] * y[0] - x[1] * y[1], x[0] * y[1] + x[1] * y[0]


def plus(x, y):
    return x[0] + y[0], x[1] + y[1]


def minus(x, y):
    return x[0] - y[0], x[1] - y[1]


def turned(x, numerator, denominator, sign):
    eighth = (8 * numerator) % (8 * denominator) / denominator
    if eighth == 0:
        return x
    if eighth == 4:
        return -x[0], -x[1]
    if eighth in (2, 6):
        if (eighth == 2) == (sign > 0):
            return -x[1], x[0]
        return x[1], -x[0]
    angle = 2.0 * math.pi * numerator / denominator
    c, s = math.cos(angle), sign * math.sin(angle)
    return x[0] * c - x[1] * s, x[1] * c + x[0] * s


def dft4(x, sign):
    a, b = plus(x[0], x[2]), minus(x[0], x[2])
    c, d = plus(x[1], x[3]), turned(minus(x[1], x[3]), 1, 4, sign)
    return [plus(a, c), plus(b, d), minus(a, c), minus(b, d)]


def dft16(x, sign):
    inner = [dft4(x[i::4], sign) for i in range(4)]
    out = [None] * 16
    for k in range(4):
        column = [turned(inner[i][k], i * k, 16, sign) for i in range(4)]
        for j, value in enumerate(dft4(column, sign)):
            out[k + 4 * j] = value
    return out


def phases_of(steps, window):
    angle = lax.bitwise_and(steps, window - 1).astype(jnp.float32) * (
        2.0 * math.pi / window
    )
    return jnp.cos(angle), -jnp.sin(angle)


def prepare(plan, fine, drift, even, odd):
    sub = lax.broadcasted_iota(jnp.int32, (SUB, LANES), 0)
    lane = lax.broadcasted_iota(jnp.int32, (SUB, LANES), 1)

    @pl.loop(0, plan.groups)
    def _(group):
        segment = 2 * ((sub // 2) * plan.groups + group) + sub % 2
        c, s = phases_of(fine * (lane + segment * LAGS), plan.window)
        drift[group, 0] = c
        drift[group, 1] = s

    @pl.loop(0, N1)
    def _(row):
        steps = jnp.full((SUB, LANES), fine * LANES * row, jnp.int32)
        c, s = phases_of(steps, plan.window)
        even[row, 0] = c
        even[row, 1] = s
        c, s = phases_of(steps + row * (plan.window // F1), plan.window)
        odd[row, 0] = c
        odd[row, 1] = s


def spread_rows(stage):
    return [
        tuple(stage[pl.ds(2 * n + part, SUB, stride=2 * N1), :] for part in range(2))
        for n in range(N1)
    ]


def turn_and_split(found, parity, forward, high, low):
    for pair in range(N1 // 2):
        both = []
        for e in (2 * pair, 2 * pair + 1):
            f1 = 2 * e + parity
            both.append(times_(found[e], (forward[f1, 0], forward[f1, 1])))
        rows = slice(parity * 128 + pair * 16, parity * 128 + pair * 16 + 16)
        for part in range(2):
            h, l = halves(jnp.concatenate([both[0][part], both[1][part]], 0))
            lanes = slice(part * LANES, (part + 1) * LANES)
            high[rows, lanes] = h
            low[rows, lanes] = l


def lanes_turned(high, low, waves, at):
    return (
        jnp.dot(high[...], waves[at], preferred_element_type=jnp.float32)
        + jnp.dot(low[...], waves[at], preferred_element_type=jnp.float32)
        + jnp.dot(high[...], waves[at + 1], preferred_element_type=jnp.float32)
    )


def signal_group(plan, group, gs, waves, forward, work, S):
    drift, even, odd, stage, high, low = work
    for z in range(4):
        start = pl.multiple_of((z * plan.groups + group) * UNIT, UNIT)
        stage[z * UNIT : (z + 1) * UNIT, :] = gs[pl.ds(start, UNIT), :].astype(
            jnp.float32
        )
    here = (drift[group, 0], drift[group, 1])
    x = [times_(v, here) for v in spread_rows(stage)]
    for parity, table in enumerate((even, odd)):
        y = [times_(x[n], (table[n, 0], table[n, 1])) for n in range(N1)]
        turn_and_split(dft16(y, -1), parity, forward, high, low)
    wide = lanes_turned(high, low, waves, 0)
    reach = plan.shifts // 2
    for f1 in range(F1):
        row = (f1 % 2) * 128 + (f1 // 2) * SUB
        for part in range(2):
            v = wide[row : row + SUB, part * LANES : (part + 1) * LANES]
            S[reach + f1, group, part] = v
            if f1 < reach:
                S[reach + f1 + F1, group, part] = pltpu.roll(v, LANES - 1, 1)
            if f1 >= F1 - reach:
                S[reach + f1 - F1, group, part] = pltpu.roll(v, 1, 1)


def reference_group(plan, group, gr, waves, forward, work, R):
    stage, stage2, high, low = work
    for z in range(4):
        start = pl.multiple_of((z * plan.groups + group) * UNIT, UNIT)
        rows = slice(z * UNIT, (z + 1) * UNIT)
        stage2[rows, :] = gr[pl.ds(start, UNIT), :].astype(jnp.float32)
        stage[rows, :] = gr[pl.ds(start + UNIT // 2, UNIT), :].astype(jnp.float32)
    now, before = spread_rows(stage), spread_rows(stage2)
    y = [plus(a, b) for a, b in zip(now, before)]
    turn_and_split(dft16(y, -1), 0, forward, high, low)
    y = [turned(minus(a, b), n, F1, -1) for n, (a, b) in enumerate(zip(now, before))]
    turn_and_split(dft16(y, -1), 1, forward, high, low)
    wide = lanes_turned(high, low, waves, 0)
    for f1 in range(F1):
        row = (f1 % 2) * 128 + (f1 // 2) * SUB
        for part in range(2):
            R[f1, group, part] = wide[
                row : row + SUB, part * LANES : (part + 1) * LANES
            ]


def fold_rows(values):
    sub = lax.broadcasted_iota(jnp.int32, (SUB, LANES), 0)
    step = 1
    while step < SUB:
        upper = (sub // step) % 2 == 1
        values = [
            jnp.where(upper, b, a) + pltpu.roll(jnp.where(upper, a, b), step, 0)
            for a, b in zip(values[::2], values[1::2])
        ]
        step *= 2
    return values[0]


def cross_spectra(plan, first, S, R, high, low):
    @pl.loop(0, F1)
    def _(f1):
        rr = [R[f1, g, 0] for g in range(plan.groups)]
        ri = [R[f1, g, 1] for g in range(plan.groups)]
        blocks = []
        for owner in range(plan.owners):
            re, im = [], []
            for i in range(SUB):
                if i >= plan.per_owner:
                    re.append(jnp.zeros((SUB, LANES), jnp.float32))
                    im.append(jnp.zeros((SUB, LANES), jnp.float32))
                    continue
                at = f1 + first + owner * plan.per_owner + i
                a = b = None
                for g in range(plan.groups):
                    sr, si = S[at, g, 0], S[at, g, 1]
                    u = sr * rr[g] + si * ri[g]
                    v = si * rr[g] - sr * ri[g]
                    a, b = (u, v) if a is None else (a + u, b + v)
                re.append(a)
                im.append(b)
            blocks.append((fold_rows(re), fold_rows(im)))
        tall = plan.owners * SUB
        rows = pl.ds(pl.multiple_of(f1 * tall, tall), tall)
        for part in range(2):
            h, l = halves(jnp.concatenate([b[part] for b in blocks], 0))
            lanes = slice(part * LANES, (part + 1) * LANES)
            high[rows, lanes] = h
            low[rows, lanes] = l


def to_lags(plan, waves, back, high, low, Z, out):
    Z[...] = lanes_turned(high, low, waves, 2)
    tall = plan.owners * SUB
    for owner in range(plan.owners):
        z = []
        for f1 in range(F1):
            rows = slice(f1 * tall + owner * SUB, f1 * tall + owner * SUB + SUB)
            v = (Z[rows, :LANES], Z[rows, LANES:])
            z.append(times_(v, (back[f1, 0], back[f1, 1])))
        half = F1 // 2
        sums = dft16([plus(z[i], z[i + half]) for i in range(half)], 1)
        gaps = dft16(
            [turned(minus(z[i], z[i + half]), i, F1, 1) for i in range(half)], 1
        )
        for e in range(N1 // 2):
            for parity, found in enumerate((sums, gaps)):
                out[2 * e + parity, owner] = jnp.concatenate(found[e], 0).astype(
                    jnp.bfloat16
                )


def compute_kernel(plan, me, gs, gr, waves, forward, back, out, *scratch):
    drift, even, odd, stage, stage2, high, low, S, R, yhigh, ylow, Z = scratch
    me = me()
    fine = me // plan.share
    first = (me % plan.share) * plan.mine
    prepare(plan, fine, drift, even, odd)

    @pl.loop(0, plan.groups)
    def _(group):
        work = (drift, even, odd, stage, high, low)
        signal_group(plan, group, gs, waves, forward, work, S)
        reference_group(plan, group, gr, waves, forward, (stage, stage2, high, low), R)

    cross_spectra(plan, first, S, R, yhigh, ylow)
    to_lags(plan, waves, back, yhigh, ylow, Z, out)


def lag_maps(plan, me, gs, gr, interpret=False):
    waves, forward, back = tables(plan)
    tall = plan.owners * SUB
    reach = plan.shifts
    f32, bf16 = jnp.float32, jnp.bfloat16
    return pl.pallas_call(
        functools.partial(compute_kernel, plan, me),
        out_shape=jax.ShapeDtypeStruct((N1, plan.owners, 2 * SUB, LANES), bf16),
        in_specs=[pl.BlockSpec(memory_space=pltpu.VMEM)] * 5,
        out_specs=pl.BlockSpec(memory_space=pltpu.VMEM),
        scratch_shapes=[
            pltpu.VMEM((plan.groups, 2, SUB, LANES), f32),
            pltpu.VMEM((N1, 2, SUB, LANES), f32),
            pltpu.VMEM((N1, 2, SUB, LANES), f32),
            pltpu.VMEM((4 * UNIT, LANES), f32),
            pltpu.VMEM((4 * UNIT, LANES), f32),
            pltpu.VMEM((F1 * SUB, 2 * LANES), bf16),
            pltpu.VMEM((F1 * SUB, 2 * LANES), bf16),
            pltpu.VMEM((F1 + reach, plan.groups, 2, SUB, LANES), f32),
            pltpu.VMEM((F1, plan.groups, 2, SUB, LANES), f32),
            pltpu.VMEM((F1 * tall, 2 * LANES), bf16),
            pltpu.VMEM((F1 * tall, 2 * LANES), bf16),
            pltpu.VMEM((F1 * tall, 2 * LANES), f32),
        ],
        compiler_params=pltpu.CompilerParams(vmem_limit_bytes=56 * 1024 * 1024),
        interpret=interpret,
    )(gs, gr, jnp.asarray(waves), jnp.asarray(forward), jnp.asarray(back))


def flipped(index, bit):
    weight = 1 << bit
    return index + weight * (1 - 2 * ((index // weight) % 2))


def spread_kernel(orders, cuts, *refs):
    count = len(orders)
    own, every = refs[:count], refs[count : 2 * count]
    send_sems, recv_sems = refs[2 * count :]
    me = lax.axis_index("tm") * cuts + lax.axis_index("dop")

    def place(index):
        return {"tm": index // cuts, "dop": index % cuts}

    barrier = pltpu.get_barrier_semaphore()
    for bit in orders[0]:
        pl.semaphore_signal(
            barrier,
            inc=1,
            device_id=place(flipped(me, bit)),
            device_id_type=pl.DeviceIdType.MESH,
        )
    pl.semaphore_wait(barrier, len(orders[0]))

    def copy(which, source, block, slot, target):
        return pltpu.make_async_remote_copy(
            src_ref=source,
            dst_ref=every[which].at[block],
            send_sem=send_sems.at[which, slot],
            recv_sem=recv_sems.at[which, block],
            device_id=place(target),
            device_id_type=pl.DeviceIdType.MESH,
        )

    sent = []
    held = [[me] for _ in orders]
    landed = [1] * count
    for step in range(len(orders[0])):
        partners = [flipped(me, order[step]) for order in orders]
        for at in range(1 << step):
            for which in range(count):
                block = held[which][at]
                mine = every[which].at[block]
                if at == 0:
                    mine = own[which]
                elif at >= landed[which]:
                    copy(which, mine, block, 0, partners[which]).wait_recv()
                    landed[which] = at + 1
                one = copy(which, mine, block, (1 << step) - 1 + at, partners[which])
                one.start()
                sent.append(one)
        for which, order in enumerate(orders):
            held[which] = held[which] + [flipped(h, order[step]) for h in held[which]]
        if step == 0:
            for which in range(count):
                every[which][pl.ds(me, 1)] = own[which][...][None]
    for which in range(count):
        for at in range(landed[which], len(held[which])):
            block = held[which][at]
            copy(which, own[which], block, 0, flipped(me, 0)).wait_recv()
    for one in sent:
        one.wait_send()


def everywhere(plan, values):
    bits = plan.devices.bit_length() - 1
    order = list(range(bits))[::-1]
    other = order[:-3] + [order[-2], order[-3], order[-1]]
    rows = values[0].shape[0]
    block = jax.ShapeDtypeStruct((plan.devices, rows, LANES), values[0].dtype)
    gathered = pl.pallas_call(
        functools.partial(spread_kernel, [order, other], plan.cuts),
        out_shape=[block] * 2,
        in_specs=[pl.BlockSpec(memory_space=pltpu.VMEM)] * 2,
        out_specs=[pl.BlockSpec(memory_space=pltpu.VMEM)] * 2,
        scratch_shapes=[
            pltpu.SemaphoreType.DMA((2, plan.devices)),
            pltpu.SemaphoreType.DMA((2, plan.devices)),
        ],
        compiler_params=pltpu.CompilerParams(collective_id=0, has_side_effects=True),
    )(*values)
    return [every.reshape(plan.devices * rows, LANES) for every in gathered]


def deal_kernel(plan, tiles, out, send_sems, recv_sems):
    cuts, times = plan.cuts, plan.times
    t, c = lax.axis_index("tm"), lax.axis_index("dop")
    me = t * cuts + c
    fine = me // plan.share
    base = (me % plan.share) * plan.owners
    mine = c // plan.owners

    barrier = pltpu.get_barrier_semaphore()
    here = fine * 0
    targets = []
    for step in range(times):
        to = (t + step) % times
        for owner in range(plan.owners):
            targets.append((step, owner, to, base + owner))
    for step, owner, to, cut in targets:
        itself = (to == t) & (cut == c)

        @pl.when(jnp.logical_not(itself))
        def _():
            pl.semaphore_signal(
                barrier, inc=1, device_id={"tm": to, "dop": cut}, device_id_type=MESH
            )

    sends_to_me = (base <= c) & (c < base + plan.owners)
    expected = plan.fine - jnp.where(sends_to_me, 1, 0)
    pl.semaphore_wait(barrier, expected)

    def copy(step, owner, to, cut):
        return pltpu.make_async_remote_copy(
            src_ref=tiles.at[to * plan.lags // LANES, owner],
            dst_ref=out.at[fine],
            send_sem=send_sems.at[step, owner],
            recv_sem=recv_sems.at[fine],
            device_id={"tm": to, "dop": cut},
            device_id_type=MESH,
        )

    for step, owner, to, cut in targets:
        itself = (to == t) & (cut == c)

        @pl.when(jnp.logical_not(itself))
        def _():
            copy(step, owner, to, cut).start()

        @pl.when(itself)
        def _():
            out[fine] = tiles[to * plan.lags // LANES, owner]

    for source in range(plan.fine):

        @pl.when((fine != source) | jnp.logical_not(sends_to_me))
        def _():
            pltpu.make_async_remote_copy(
                src_ref=tiles.at[0, 0],
                dst_ref=out.at[source],
                send_sem=send_sems.at[0, 0],
                recv_sem=recv_sems.at[source],
                device_id={"tm": t, "dop": c},
                device_id_type=MESH,
            ).wait_recv()

    for step, owner, to, cut in targets:
        itself = (to == t) & (cut == c)

        @pl.when(jnp.logical_not(itself))
        def _():
            copy(step, owner, to, cut).wait_send()


def dealt(plan, tiles):
    return pl.pallas_call(
        functools.partial(deal_kernel, plan),
        out_shape=jax.ShapeDtypeStruct((plan.fine, 2 * SUB, LANES), tiles.dtype),
        in_specs=[pl.BlockSpec(memory_space=pltpu.VMEM)],
        out_specs=pl.BlockSpec(memory_space=pltpu.VMEM),
        scratch_shapes=[
            pltpu.SemaphoreType.DMA((plan.times, plan.owners)),
            pltpu.SemaphoreType.DMA((plan.fine,)),
        ],
        compiler_params=pltpu.CompilerParams(collective_id=1, has_side_effects=True),
    )(tiles)


def order_of(plan):
    bins = F // plan.cuts
    order = np.zeros((plan.fine, 2, SUB, 2, bins), np.float32)
    for fine in range(plan.fine):
        for part in range(2):
            for i in range(plan.per_owner):
                order[fine, part, i, part, plan.fine * i + fine] = 1.0
    return order.reshape(plan.fine * 2 * SUB, 2 * bins).astype(jnp.bfloat16)


def settle_kernel(plan, tiles, order, out):
    rows = plan.fine * 2 * SUB
    wide = lax.dot_general(
        tiles[...].reshape(rows, LANES),
        order[...],
        (((0,), (0,)), ((), ())),
        preferred_element_type=jnp.float32,
    )
    bins = F // plan.cuts
    if plan.lags < LANES:
        pieces = LANES // plan.lags
        which = lax.axis_index("tm") % pieces
        kept = wide[: plan.lags]
        for piece in range(1, pieces):
            kept = jnp.where(
                which == piece, wide[piece * plan.lags : (piece + 1) * plan.lags], kept
            )
        wide = kept
    out[:, 0, :] = wide[:, :bins]
    out[:, 1, :] = wide[:, bins:]


def settled(plan, tiles):
    return pl.pallas_call(
        functools.partial(settle_kernel, plan),
        out_shape=jax.ShapeDtypeStruct((plan.lags, 2, F // plan.cuts), jnp.float32),
        in_specs=[pl.BlockSpec(memory_space=pltpu.VMEM)] * 2,
        out_specs=pl.BlockSpec(memory_space=pltpu.VMEM),
    )(tiles, jnp.asarray(order_of(plan)))


def paired_rows(x):
    samples = x.shape[1] * x.shape[2]
    split = x.reshape(2, samples // LANES, LANES).transpose(1, 0, 2)
    return split.reshape(2 * samples // LANES, LANES)


def on_device(surveillance, reference_signal):
    times, cuts = lax.axis_size("tm"), lax.axis_size("dop")
    samples = surveillance.shape[1] * surveillance.shape[2]
    plan = Plan(times, cuts, samples * times * cuts)
    me = lambda: lax.axis_index("tm") * cuts + lax.axis_index("dop")
    gs, gr = everywhere(plan, [paired_rows(surveillance), paired_rows(reference_signal)])
    gr = jnp.pad(gr, ((UNIT // 2, 0), (0, 0)))
    return settled(plan, dealt(plan, lag_maps(plan, me, gs, gr)))


def solution(mesh):
    return jax.shard_map(
        on_device,
        mesh=mesh,
        in_specs=(P(None, "tm", "dop"), P(None, "tm", "dop")),
        out_specs=P("tm", None, "dop"),
        check_vma=False,
    )
```

```python
import functools
import math

import jax
import jax.numpy as jnp
import numpy as np
from jax import lax
from jax.experimental import pallas as pl
from jax.experimental.pallas import tpu as pltpu
from jax.sharding import PartitionSpec as P

F = 512
LAGS = 2048
LANES = 128
SUB = 8
POINTS = 2 * LAGS
N1 = LAGS // LANES
F1 = POINTS // LANES
UNIT = 2 * N1 * 2
MESH = pl.DeviceIdType.MESH


class Plan:
    def __init__(self, times, cuts, window):
        self.times, self.cuts, self.window = times, cuts, window
        self.devices = times * cuts
        self.units = window // (2 * LAGS)
        self.groups = self.units // 4
        self.fine = window // POINTS
        self.shifts = F // self.fine
        self.share = self.devices // self.fine
        self.mine = self.shifts // self.share
        self.per_owner = self.shifts // cuts
        self.owners = self.mine // self.per_owner
        self.lags = LAGS // times


def halves(x):
    high = x.astype(jnp.bfloat16)
    low = (x - high.astype(jnp.float32)).astype(jnp.bfloat16)
    return high, low


def tables(plan):
    a = np.arange(LANES)
    angle = 2.0 * np.pi / LANES * np.mod(a[:, None] * a[None, :], LANES)
    c, s = np.cos(angle), np.sin(angle)
    waves = []
    for sign in (-1.0, 1.0):
        full = np.block([[c, sign * s], [-sign * s, c]])
        high = full.astype(jnp.bfloat16)
        low = (full - high.astype(np.float64)).astype(jnp.bfloat16)
        waves += [high, low]
    turn = 2.0 * np.pi / POINTS * np.arange(F1)[:, None] * a[None, :]
    turns = np.stack([np.cos(turn), -np.sin(turn)], 1)
    sign = np.where(
        (np.arange(F1)[:, None] * np.arange(SUB)[None, :]) % 2 == 1, -1.0, 1.0
    )
    forward = (turns[:, :, None, :] * sign[:, None, :, None]).astype(np.float32)
    scale = 1.0 / (POINTS * math.sqrt(plan.window))
    back = (np.stack([np.cos(turn), np.sin(turn)], 1) * scale).astype(np.float32)
    back = np.broadcast_to(back[:, :, None, :], (F1, 2, SUB, LANES)).copy()
    return np.stack(waves), forward, back


def times_(x, y):
    return x[0] * y[0] - x[1] * y[1], x[0] * y[1] + x[1] * y[0]


def plus(x, y):
    return x[0] + y[0], x[1] + y[1]


def minus(x, y):
    return x[0] - y[0], x[1] - y[1]


def turned(x, numerator, denominator, sign):
    eighth = (8 * numerator) % (8 * denominator) / denominator
    if eighth == 0:
        return x
    if eighth == 4:
        return -x[0], -x[1]
    if eighth in (2, 6):
        if (eighth == 2) == (sign > 0):
            return -x[1], x[0]
        return x[1], -x[0]
    angle = 2.0 * math.pi * numerator / denominator
    c, s = math.cos(angle), sign * math.sin(angle)
    return x[0] * c - x[1] * s, x[1] * c + x[0] * s


def dft4(x, sign):
    a, b = plus(x[0], x[2]), minus(x[0], x[2])
    c, d = plus(x[1], x[3]), turned(minus(x[1], x[3]), 1, 4, sign)
    return [plus(a, c), plus(b, d), minus(a, c), minus(b, d)]


def dft16(x, sign):
    inner = [dft4(x[i::4], sign) for i in range(4)]
    out = [None] * 16
    for k in range(4):
        column = [turned(inner[i][k], i * k, 16, sign) for i in range(4)]
        for j, value in enumerate(dft4(column, sign)):
            out[k + 4 * j] = value
    return out


def phases_of(steps, window):
    angle = lax.bitwise_and(steps, window - 1).astype(jnp.float32) * (
        2.0 * math.pi / window
    )
    return jnp.cos(angle), -jnp.sin(angle)


def prepare(plan, fine, drift, even, odd):
    sub = lax.broadcasted_iota(jnp.int32, (SUB, LANES), 0)
    lane = lax.broadcasted_iota(jnp.int32, (SUB, LANES), 1)

    @pl.loop(0, plan.groups)
    def _(group):
        segment = 2 * ((sub // 2) * plan.groups + group) + sub % 2
        c, s = phases_of(fine * (lane + segment * LAGS), plan.window)
        drift[group, 0] = c
        drift[group, 1] = s

    @pl.loop(0, N1)
    def _(row):
        steps = jnp.full((SUB, LANES), fine * LANES * row, jnp.int32)
        c, s = phases_of(steps, plan.window)
        even[row, 0] = c
        even[row, 1] = s
        c, s = phases_of(steps + row * (plan.window // F1), plan.window)
        odd[row, 0] = c
        odd[row, 1] = s


def spread_rows(stage):
    return [
        tuple(stage[pl.ds(2 * n + part, SUB, stride=2 * N1), :] for part in range(2))
        for n in range(N1)
    ]


def turn_and_split(found, parity, forward, high, low):
    for pair in range(N1 // 2):
        both = []
        for e in (2 * pair, 2 * pair + 1):
            f1 = 2 * e + parity
            both.append(times_(found[e], (forward[f1, 0], forward[f1, 1])))
        rows = slice(parity * 128 + pair * 16, parity * 128 + pair * 16 + 16)
        for part in range(2):
            h, l = halves(jnp.concatenate([both[0][part], both[1][part]], 0))
            lanes = slice(part * LANES, (part + 1) * LANES)
            high[rows, lanes] = h
            low[rows, lanes] = l


def lanes_turned(high, low, waves, at):
    return (
        jnp.dot(high[...], waves[at], preferred_element_type=jnp.float32)
        + jnp.dot(low[...], waves[at], preferred_element_type=jnp.float32)
        + jnp.dot(high[...], waves[at + 1], preferred_element_type=jnp.float32)
    )


def signal_group(plan, group, gs, waves, forward, work, S):
    drift, even, odd, stage, high, low = work
    for z in range(4):
        start = pl.multiple_of((z * plan.groups + group) * UNIT, UNIT)
        stage[z * UNIT : (z + 1) * UNIT, :] = gs[pl.ds(start, UNIT), :].astype(
            jnp.float32
        )
    here = (drift[group, 0], drift[group, 1])
    x = [times_(v, here) for v in spread_rows(stage)]
    for parity, table in enumerate((even, odd)):
        y = [times_(x[n], (table[n, 0], table[n, 1])) for n in range(N1)]
        turn_and_split(dft16(y, -1), parity, forward, high, low)
    wide = lanes_turned(high, low, waves, 0)
    reach = plan.shifts // 2
    for f1 in range(F1):
        row = (f1 % 2) * 128 + (f1 // 2) * SUB
        for part in range(2):
            v = wide[row : row + SUB, part * LANES : (part + 1) * LANES]
            S[reach + f1, group, part] = v
            if f1 < reach:
                S[reach + f1 + F1, group, part] = pltpu.roll(v, LANES - 1, 1)
            if f1 >= F1 - reach:
                S[reach + f1 - F1, group, part] = pltpu.roll(v, 1, 1)


def reference_group(plan, group, gr, waves, forward, work, R):
    stage, stage2, high, low = work
    for z in range(4):
        start = pl.multiple_of((z * plan.groups + group) * UNIT, UNIT)
        rows = slice(z * UNIT, (z + 1) * UNIT)
        stage2[rows, :] = gr[pl.ds(start, UNIT), :].astype(jnp.float32)
        stage[rows, :] = gr[pl.ds(start + UNIT // 2, UNIT), :].astype(jnp.float32)
    now, before = spread_rows(stage), spread_rows(stage2)
    y = [plus(a, b) for a, b in zip(now, before)]
    turn_and_split(dft16(y, -1), 0, forward, high, low)
    y = [turned(minus(a, b), n, F1, -1) for n, (a, b) in enumerate(zip(now, before))]
    turn_and_split(dft16(y, -1), 1, forward, high, low)
    wide = lanes_turned(high, low, waves, 0)
    for f1 in range(F1):
        row = (f1 % 2) * 128 + (f1 // 2) * SUB
        for part in range(2):
            R[f1, group, part] = wide[
                row : row + SUB, part * LANES : (part + 1) * LANES
            ]


def fold_rows(values):
    sub = lax.broadcasted_iota(jnp.int32, (SUB, LANES), 0)
    step = 1
    while step < SUB:
        upper = (sub // step) % 2 == 1
        values = [
            jnp.where(upper, b, a) + pltpu.roll(jnp.where(upper, a, b), step, 0)
            for a, b in zip(values[::2], values[1::2])
        ]
        step *= 2
    return values[0]


def cross_spectra(plan, first, S, R, high, low):
    @pl.loop(0, F1)
    def _(f1):
        rr = [R[f1, g, 0] for g in range(plan.groups)]
        ri = [R[f1, g, 1] for g in range(plan.groups)]
        blocks = []
        for owner in range(plan.owners):
            re, im = [], []
            for i in range(SUB):
                if i >= plan.per_owner:
                    re.append(jnp.zeros((SUB, LANES), jnp.float32))
                    im.append(jnp.zeros((SUB, LANES), jnp.float32))
                    continue
                at = f1 + first + owner * plan.per_owner + i
                a = b = None
                for g in range(plan.groups):
                    sr, si = S[at, g, 0], S[at, g, 1]
                    u = sr * rr[g] + si * ri[g]
                    v = si * rr[g] - sr * ri[g]
                    a, b = (u, v) if a is None else (a + u, b + v)
                re.append(a)
                im.append(b)
            blocks.append((fold_rows(re), fold_rows(im)))
        tall = plan.owners * SUB
        rows = pl.ds(pl.multiple_of(f1 * tall, tall), tall)
        for part in range(2):
            h, l = halves(jnp.concatenate([b[part] for b in blocks], 0))
            lanes = slice(part * LANES, (part + 1) * LANES)
            high[rows, lanes] = h
            low[rows, lanes] = l


def to_lags(plan, waves, back, high, low, Z, out):
    Z[...] = lanes_turned(high, low, waves, 2)
    tall = plan.owners * SUB
    for owner in range(plan.owners):
        z = []
        for f1 in range(F1):
            rows = slice(f1 * tall + owner * SUB, f1 * tall + owner * SUB + SUB)
            v = (Z[rows, :LANES], Z[rows, LANES:])
            z.append(times_(v, (back[f1, 0], back[f1, 1])))
        half = F1 // 2
        sums = dft16([plus(z[i], z[i + half]) for i in range(half)], 1)
        gaps = dft16(
            [turned(minus(z[i], z[i + half]), i, F1, 1) for i in range(half)], 1
        )
        for e in range(N1 // 2):
            for parity, found in enumerate((sums, gaps)):
                out[2 * e + parity, owner] = jnp.concatenate(found[e], 0).astype(
                    jnp.bfloat16
                )


def across(plan, own, every, sems, prepared):
    send_sems, recv_sems = sems
    cuts, far = plan.cuts, plan.times // 4
    t, c = lax.axis_index("tm"), lax.axis_index("dop")
    z, near = t // 4, t % 4
    beside = (flipped(near, 0), flipped(near, 1))
    others = [flipped_by(z, k) for k in range(1, far)]
    fellows = [flipped_by(c, k) for k in range(1, cuts)]

    partners = [(z * 4 + n, c) for n in beside]
    partners += [(other * 4 + near, c) for other in others]
    partners += [(t, fellow) for fellow in fellows]
    barrier = pltpu.get_barrier_semaphore()
    for to, cut in partners:
        pl.semaphore_signal(
            barrier, inc=1, device_id={"tm": to, "dop": cut}, device_id_type=MESH
        )
    pl.semaphore_wait(barrier, len(partners))

    sent = []
    rows = own[0].shape[0]
    pad = (0, UNIT // 2)

    def place(which, source):
        start = pl.multiple_of(source * rows, rows) + pad[which]
        return every[which].at[pl.ds(pl.multiple_of(start, 16), rows)]

    def copy(which, source, src, to, cut, slot):
        return pltpu.make_async_remote_copy(
            src_ref=src,
            dst_ref=place(which, source),
            send_sem=send_sems.at[slot],
            recv_sem=recv_sems.at[which, source],
            device_id={"tm": to, "dop": cut},
            device_id_type=MESH,
        )

    def send(which, source, to, cut, mine=False):
        src = own[which] if mine else place(which, source)
        one = copy(which, source, src, to, cut, len(sent))
        one.start()
        sent.append(one)

    def landed(which, source):
        copy(which, source, own[which], t, c, 0).wait_recv()

    me = t * cuts + c
    for other in others[::-1]:
        for which in range(2):
            send(which, me, other * 4 + near, c, True)
    for n in beside:
        for which in range(2):
            send(which, me, z * 4 + n, c, True)
    for fellow in fellows:
        for which in range(2):
            send(which, me, t, fellow, True)
    for which in range(2):
        every[which][pl.ds(pl.multiple_of(me * rows + pad[which], 16), rows)] = own[
            which
        ][...]
    prepared()

    corner = flipped(beside[0], 1)
    levels = [z] + others
    for k in range(far + 1):
        if k < far:
            level = levels[k]
            if k > 0:
                source = (level * 4 + near) * cuts + c
                for which in range(2):
                    landed(which, source)
                    for n in beside:
                        send(which, source, z * 4 + n, c)
                    for fellow in fellows:
                        send(which, source, t, fellow)
            for side in range(2):
                source = (level * 4 + beside[side]) * cuts + c
                for which in range(2):
                    landed(which, source)
                    if which == side:
                        send(which, source, z * 4 + beside[1 - side], c)
                    for fellow in fellows:
                        send(which, source, t, fellow)
        if k > 0:
            source = (levels[k - 1] * 4 + corner) * cuts + c
            for which in range(2):
                landed(which, source)
                for fellow in fellows:
                    send(which, source, t, fellow)
    for fellow in fellows:
        for level in levels:
            for n in (near, beside[0], beside[1], corner):
                for which in range(2):
                    landed(which, (level * 4 + n) * cuts + fellow)
    return sent


def sends_needed(plan):
    far, fellows = plan.times // 4, plan.cuts - 1
    return 2 * (far - 1 + 2 + fellows) + 2 * (far - 1) * (2 + fellows) + (
        far * (2 + 6 * fellows)
    )


def deal(plan, tiles, out, sems):
    send_sems, recv_sems = sems
    times = plan.times
    t, c = lax.axis_index("tm"), lax.axis_index("dop")
    me = t * plan.cuts + c
    fine = me // plan.share
    base = (me % plan.share) * plan.owners
    to_me = (base <= c) & (c < base + plan.owners)

    def copy(step, owner):
        to = flipped_by(t, step)
        return pltpu.make_async_remote_copy(
            src_ref=tiles.at[to * plan.lags // LANES, owner],
            dst_ref=out.at[fine],
            send_sem=send_sems.at[step, owner],
            recv_sem=recv_sems.at[fine],
            device_id={"tm": to, "dop": base + owner},
            device_id_type=MESH,
        )

    for step in range(times - 1, 0, -1):
        for owner in range(plan.owners):
            copy(step, owner).start()
    for owner in range(plan.owners):
        itself = base + owner == c

        @pl.when(jnp.logical_not(itself))
        def _():
            copy(0, owner).start()

        @pl.when(itself)
        def _():
            out[fine] = tiles[t * plan.lags // LANES, owner]

    for source in range(plan.fine):

        @pl.when((fine != source) | jnp.logical_not(to_me))
        def _():
            pltpu.make_async_remote_copy(
                src_ref=tiles.at[0, 0],
                dst_ref=out.at[source],
                send_sem=send_sems.at[0, 0],
                recv_sem=recv_sems.at[source],
                device_id={"tm": t, "dop": c},
                device_id_type=MESH,
            ).wait_recv()

    for step in range(1, times):
        for owner in range(plan.owners):
            copy(step, owner).wait_send()
    for owner in range(plan.owners):

        @pl.when(base + owner != c)
        def _():
            copy(0, owner).wait_send()


def whole_kernel(plan, s, r, waves_at, forward_at, back_at, out, *scratch):
    (gs, gr, waves, forward, back, tiles) = scratch[:6]
    drift, even, odd, stage, stage2, high, low, S, R, yhigh, ylow, Z = scratch[6:18]
    load_sems, gather_sems, deal_sems = scratch[18], scratch[19:21], scratch[21:23]
    me = lax.axis_index("tm") * plan.cuts + lax.axis_index("dop")
    fine = me // plan.share
    first = (me % plan.share) * plan.mine
    loads = [
        pltpu.make_async_copy(source, target, load_sems.at[i])
        for i, (source, target) in enumerate(
            ((waves_at, waves), (forward_at, forward), (back_at, back))
        )
    ]

    def prepared():
        for load in loads:
            load.start()
        gr[: UNIT // 2, :] = jnp.zeros((UNIT // 2, LANES), jnp.bfloat16)
        prepare(plan, fine, drift, even, odd)

    sent = across(plan, (s, r), (gs, gr), gather_sems, prepared)
    for load in loads:
        load.wait()

    @pl.loop(0, plan.groups)
    def _(group):
        work = (drift, even, odd, stage, high, low)
        signal_group(plan, group, gs, waves, forward, work, S)
        reference_group(plan, group, gr, waves, forward, (stage, stage2, high, low), R)

    cross_spectra(plan, first, S, R, yhigh, ylow)
    to_lags(plan, waves, back, yhigh, ylow, Z, tiles)
    deal(plan, tiles, out, deal_sems)
    for one in sent:
        one.wait_send()


def dealt_maps(plan, s, r):
    waves, forward, back = tables(plan)
    tall = plan.owners * SUB
    f32, bf16 = jnp.float32, jnp.bfloat16
    samples = 2 * plan.window // LANES
    return pl.pallas_call(
        functools.partial(whole_kernel, plan),
        out_shape=jax.ShapeDtypeStruct((plan.fine, 2 * SUB, LANES), bf16),
        in_specs=[pl.BlockSpec(memory_space=pltpu.VMEM)] * 2
        + [pl.BlockSpec(memory_space=pl.ANY)] * 3,
        out_specs=pl.BlockSpec(memory_space=pltpu.VMEM),
        scratch_shapes=[
            pltpu.VMEM((samples, LANES), bf16),
            pltpu.VMEM((samples + UNIT // 2, LANES), bf16),
            pltpu.VMEM(waves.shape, bf16),
            pltpu.VMEM(forward.shape, f32),
            pltpu.VMEM(back.shape, f32),
            pltpu.VMEM((N1, plan.owners, 2 * SUB, LANES), bf16),
            pltpu.VMEM((plan.groups, 2, SUB, LANES), f32),
            pltpu.VMEM((N1, 2, SUB, LANES), f32),
            pltpu.VMEM((N1, 2, SUB, LANES), f32),
            pltpu.VMEM((4 * UNIT, LANES), f32),
            pltpu.VMEM((4 * UNIT, LANES), f32),
            pltpu.VMEM((F1 * SUB, 2 * LANES), bf16),
            pltpu.VMEM((F1 * SUB, 2 * LANES), bf16),
            pltpu.VMEM((F1 + plan.shifts, plan.groups, 2, SUB, LANES), f32),
            pltpu.VMEM((F1, plan.groups, 2, SUB, LANES), f32),
            pltpu.VMEM((F1 * tall, 2 * LANES), bf16),
            pltpu.VMEM((F1 * tall, 2 * LANES), bf16),
            pltpu.VMEM((F1 * tall, 2 * LANES), f32),
            pltpu.SemaphoreType.DMA((3,)),
            pltpu.SemaphoreType.DMA((sends_needed(plan),)),
            pltpu.SemaphoreType.DMA((2, plan.devices)),
            pltpu.SemaphoreType.DMA((plan.times, plan.owners)),
            pltpu.SemaphoreType.DMA((plan.fine,)),
        ],
        compiler_params=pltpu.CompilerParams(
            collective_id=0,
            has_side_effects=True,
            vmem_limit_bytes=56 * 1024 * 1024,
        ),
    )(s, r, jnp.asarray(waves), jnp.asarray(forward), jnp.asarray(back))


def flipped(index, bit):
    weight = 1 << bit
    return index + weight * (1 - 2 * ((index // weight) % 2))


def flipped_by(index, mask):
    for bit in range(mask.bit_length()):
        if mask >> bit & 1:
            index = flipped(index, bit)
    return index


def order_of(plan):
    bins = F // plan.cuts
    order = np.zeros((plan.fine, 2, SUB, 2, bins), np.float32)
    for fine in range(plan.fine):
        for part in range(2):
            for i in range(plan.per_owner):
                order[fine, part, i, part, plan.fine * i + fine] = 1.0
    return order.reshape(plan.fine * 2 * SUB, 2 * bins).astype(jnp.bfloat16)


def settle_kernel(plan, tiles, order, out):
    rows = plan.fine * 2 * SUB
    wide = lax.dot_general(
        tiles[...].reshape(rows, LANES),
        order[...],
        (((0,), (0,)), ((), ())),
        preferred_element_type=jnp.float32,
    )
    bins = F // plan.cuts
    if plan.lags < LANES:
        pieces = LANES // plan.lags
        which = lax.axis_index("tm") % pieces
        kept = wide[: plan.lags]
        for piece in range(1, pieces):
            kept = jnp.where(
                which == piece, wide[piece * plan.lags : (piece + 1) * plan.lags], kept
            )
        wide = kept
    out[:, 0, :] = wide[:, :bins]
    out[:, 1, :] = wide[:, bins:]


def settled(plan, tiles):
    return pl.pallas_call(
        functools.partial(settle_kernel, plan),
        out_shape=jax.ShapeDtypeStruct((plan.lags, 2, F // plan.cuts), jnp.float32),
        in_specs=[pl.BlockSpec(memory_space=pltpu.VMEM)] * 2,
        out_specs=pl.BlockSpec(memory_space=pltpu.VMEM),
    )(tiles, jnp.asarray(order_of(plan)))


def paired_rows(x):
    samples = x.shape[1] * x.shape[2]
    split = x.reshape(2, samples // LANES, LANES).transpose(1, 0, 2)
    return split.reshape(2 * samples // LANES, LANES)


def on_device(surveillance, reference_signal):
    times, cuts = lax.axis_size("tm"), lax.axis_size("dop")
    samples = surveillance.shape[1] * surveillance.shape[2]
    plan = Plan(times, cuts, samples * times * cuts)
    tiles = dealt_maps(plan, paired_rows(surveillance), paired_rows(reference_signal))
    return settled(plan, tiles)


def solution(mesh):
    return jax.shard_map(
        on_device,
        mesh=mesh,
        in_specs=(P(None, "tm", "dop"), P(None, "tm", "dop")),
        out_specs=P("tm", None, "dop"),
        check_vma=False,
    )
```

```python
import functools
import math

import jax
import jax.numpy as jnp
import numpy as np
from jax import lax
from jax.experimental import pallas as pl
from jax.experimental.pallas import tpu as pltpu
from jax.sharding import PartitionSpec as P

F = 512
LAGS = 2048
LANES = 128
SUB = 8
POINTS = 2 * LAGS
N1 = LAGS // LANES
F1 = POINTS // LANES
ROWS = 2 * N1
GROUP = SUB * ROWS
APART = ROWS + 1
MESH = pl.DeviceIdType.MESH


class Plan:
    def __init__(self, times, cuts, window):
        self.times, self.cuts, self.window = times, cuts, window
        self.devices = times * cuts
        self.groups = window // (SUB * LAGS)
        self.far = times // 4
        self.fine = window // POINTS
        self.shifts = F // self.fine
        self.share = self.devices // self.fine
        self.mine = self.shifts // self.share
        self.per_owner = self.shifts // cuts
        self.owners = self.mine // self.per_owner
        self.lags = LAGS // times


def halves(x):
    high = x.astype(jnp.bfloat16)
    low = (x - high.astype(jnp.float32)).astype(jnp.bfloat16)
    return high, low


def tables(plan):
    a = np.arange(LANES)
    angle = 2.0 * np.pi / LANES * np.mod(a[:, None] * a[None, :], LANES)
    c, s = np.cos(angle), np.sin(angle)
    waves = []
    for sign in (-1.0, 1.0):
        full = np.block([[c, sign * s], [-sign * s, c]])
        high = full.astype(jnp.bfloat16)
        low = (full - high.astype(np.float64)).astype(jnp.bfloat16)
        waves += [high, low]
    turn = 2.0 * np.pi / POINTS * np.arange(F1)[:, None] * a[None, :]
    turns = np.stack([np.cos(turn), -np.sin(turn)], 1)
    sign = np.where(
        (np.arange(F1)[:, None] * np.arange(SUB)[None, :]) % 2 == 1, -1.0, 1.0
    )
    forward = (turns[:, :, None, :] * sign[:, None, :, None]).astype(np.float32)
    scale = 1.0 / (POINTS * math.sqrt(plan.window))
    back = (np.stack([np.cos(turn), np.sin(turn)], 1) * scale).astype(np.float32)
    back = np.broadcast_to(back[:, :, None, :], (F1, 2, SUB, LANES)).copy()
    return np.stack(waves), forward, back


def times_(x, y):
    return x[0] * y[0] - x[1] * y[1], x[0] * y[1] + x[1] * y[0]


def plus(x, y):
    return x[0] + y[0], x[1] + y[1]


def minus(x, y):
    return x[0] - y[0], x[1] - y[1]


def turned(x, numerator, denominator, sign):
    eighth = (8 * numerator) % (8 * denominator) / denominator
    if eighth == 0:
        return x
    if eighth == 4:
        return -x[0], -x[1]
    if eighth in (2, 6):
        if (eighth == 2) == (sign > 0):
            return -x[1], x[0]
        return x[1], -x[0]
    angle = 2.0 * math.pi * numerator / denominator
    c, s = math.cos(angle), sign * math.sin(angle)
    return x[0] * c - x[1] * s, x[1] * c + x[0] * s


def dft4(x, sign):
    a, b = plus(x[0], x[2]), minus(x[0], x[2])
    c, d = plus(x[1], x[3]), turned(minus(x[1], x[3]), 1, 4, sign)
    return [plus(a, c), plus(b, d), minus(a, c), minus(b, d)]


def dft16(x, sign):
    inner = [dft4(x[i::4], sign) for i in range(4)]
    out = [None] * 16
    for k in range(4):
        column = [turned(inner[i][k], i * k, 16, sign) for i in range(4)]
        for j, value in enumerate(dft4(column, sign)):
            out[k + 4 * j] = value
    return out


def phases_of(steps, window):
    angle = lax.bitwise_and(steps, window - 1).astype(jnp.float32) * (
        2.0 * math.pi / window
    )
    return jnp.cos(angle), -jnp.sin(angle)


def prepare(plan, fine, drift, even, odd):
    sub = lax.broadcasted_iota(jnp.int32, (SUB, LANES), 0)
    lane = lax.broadcasted_iota(jnp.int32, (SUB, LANES), 1)

    @pl.loop(0, plan.groups)
    def _(group):
        segment = SUB * group + sub
        c, s = phases_of(fine * (lane + segment * LAGS), plan.window)
        drift[group, 0] = c
        drift[group, 1] = s

    @pl.loop(0, N1)
    def _(row):
        steps = jnp.full((SUB, LANES), fine * LANES * row, jnp.int32)
        c, s = phases_of(steps, plan.window)
        even[row, 0] = c
        even[row, 1] = s
        c, s = phases_of(steps + row * (plan.window // F1), plan.window)
        odd[row, 0] = c
        odd[row, 1] = s


def staged(rows, stage):
    for i in range(rows.shape[0] // ROWS):
        stage[i * APART : i * APART + ROWS, :] = rows[
            i * ROWS : (i + 1) * ROWS, :
        ].astype(jnp.float32)


def spread_rows(stage, skip=0):
    first = skip * APART
    return [
        tuple(
            stage[pl.ds(first + 2 * n + part, SUB, stride=APART), :]
            for part in range(2)
        )
        for n in range(N1)
    ]


def turn_and_split(found, parity, forward, high, low):
    for pair in range(N1 // 2):
        both = []
        for e in (2 * pair, 2 * pair + 1):
            f1 = 2 * e + parity
            both.append(times_(found[e], (forward[f1, 0], forward[f1, 1])))
        rows = slice(parity * 128 + pair * 16, parity * 128 + pair * 16 + 16)
        for part in range(2):
            h, l = halves(jnp.concatenate([both[0][part], both[1][part]], 0))
            lanes = slice(part * LANES, (part + 1) * LANES)
            high[rows, lanes] = h
            low[rows, lanes] = l


def lanes_turned(high, low, waves, at):
    return (
        jnp.dot(high[...], waves[at], preferred_element_type=jnp.float32)
        + jnp.dot(low[...], waves[at], preferred_element_type=jnp.float32)
        + jnp.dot(high[...], waves[at + 1], preferred_element_type=jnp.float32)
    )


def signal_group(plan, group, slot, gs, waves, forward, work, S):
    drift, even, odd, stage, high, low = work
    start = pl.multiple_of(group * GROUP, GROUP)
    staged(gs[pl.ds(start, GROUP), :], stage)
    here = (drift[group, 0], drift[group, 1])
    x = [times_(v, here) for v in spread_rows(stage)]
    for parity, table in enumerate((even, odd)):
        y = [times_(x[n], (table[n, 0], table[n, 1])) for n in range(N1)]
        turn_and_split(dft16(y, -1), parity, forward, high, low)
    wide = lanes_turned(high, low, waves, 0)
    reach = plan.shifts // 2
    for f1 in range(F1):
        row = (f1 % 2) * 128 + (f1 // 2) * SUB
        for part in range(2):
            v = wide[row : row + SUB, part * LANES : (part + 1) * LANES]
            S[slot, reach + f1, part] = v
            if f1 < reach:
                S[slot, reach + f1 + F1, part] = pltpu.roll(v, LANES - 1, 1)
            if f1 >= F1 - reach:
                S[slot, reach + f1 - F1, part] = pltpu.roll(v, 1, 1)


def reference_group(plan, group, slot, gr, waves, forward, work, R):
    stage, high, low = work
    start = pl.multiple_of(group * GROUP, GROUP)
    staged(gr[pl.ds(start, GROUP + ROWS), :], stage)
    before, now = spread_rows(stage), spread_rows(stage, 1)
    y = [plus(a, b) for a, b in zip(now, before)]
    turn_and_split(dft16(y, -1), 0, forward, high, low)
    y = [turned(minus(a, b), n, F1, -1) for n, (a, b) in enumerate(zip(now, before))]
    turn_and_split(dft16(y, -1), 1, forward, high, low)
    wide = lanes_turned(high, low, waves, 0)
    for f1 in range(F1):
        row = (f1 % 2) * 128 + (f1 // 2) * SUB
        for part in range(2):
            R[slot, f1, part] = wide[
                row : row + SUB, part * LANES : (part + 1) * LANES
            ]


def fold_rows(values):
    sub = lax.broadcasted_iota(jnp.int32, (SUB, LANES), 0)
    step = 1
    while step < SUB:
        upper = (sub // step) % 2 == 1
        values = [
            jnp.where(upper, b, a) + pltpu.roll(jnp.where(upper, a, b), step, 0)
            for a, b in zip(values[::2], values[1::2])
        ]
        step *= 2
    return values[0]


def product(plan, first, f1, owner, i, slots, S, R, held, start):
    at = f1 + first + owner * plan.per_owner + i
    index = owner * plan.per_owner + i
    a = b = None
    if not start:
        a, b = held[f1, index, 0], held[f1, index, 1]
    for slot in range(slots):
        sr, si = S[slot, at, 0], S[slot, at, 1]
        rr, ri = R[slot, f1, 0], R[slot, f1, 1]
        u = sr * rr + si * ri
        v = si * rr - sr * ri
        a, b = (u, v) if a is None else (a + u, b + v)
    return a, b


def add_spectra(plan, first, slots, S, R, held, start):
    step = 4

    @pl.loop(0, F1 // step)
    def _(block):
        for k in range(step):
            f1 = block * step + k
            for owner in range(plan.owners):
                for i in range(plan.per_owner):
                    a, b = product(plan, first, f1, owner, i, slots, S, R, held, start)
                    index = owner * plan.per_owner + i
                    held[f1, index, 0] = a
                    held[f1, index, 1] = b


def last_spectra(plan, first, slots, S, R, held, high, low):
    @pl.loop(0, F1)
    def _(f1):
        blocks = []
        for owner in range(plan.owners):
            found = []
            for i in range(SUB):
                if i < plan.per_owner:
                    found.append(
                        product(plan, first, f1, owner, i, slots, S, R, held, False)
                    )
                else:
                    found.append((jnp.zeros((SUB, LANES), jnp.float32),) * 2)
            blocks.append([fold_rows([v[part] for v in found]) for part in range(2)])
        tall = plan.owners * SUB
        rows = pl.ds(pl.multiple_of(f1 * tall, tall), tall)
        for part in range(2):
            h, l = halves(jnp.concatenate([b[part] for b in blocks], 0))
            lanes = slice(part * LANES, (part + 1) * LANES)
            high[rows, lanes] = h
            low[rows, lanes] = l


def to_lags(plan, waves, back, high, low, Z, out):
    Z[...] = lanes_turned(high, low, waves, 2)
    tall = plan.owners * SUB
    for owner in range(plan.owners):
        z = []
        for f1 in range(F1):
            rows = slice(f1 * tall + owner * SUB, f1 * tall + owner * SUB + SUB)
            v = (Z[rows, :LANES], Z[rows, LANES:])
            z.append(times_(v, (back[f1, 0], back[f1, 1])))
        half = F1 // 2
        sums = dft16([plus(z[i], z[i + half]) for i in range(half)], 1)
        gaps = dft16(
            [turned(minus(z[i], z[i + half]), i, F1, 1) for i in range(half)], 1
        )
        for e in range(N1 // 2):
            for parity, found in enumerate((sums, gaps)):
                out[2 * e + parity, owner] = jnp.concatenate(found[e], 0).astype(
                    jnp.bfloat16
                )


def schedule(plan):
    far = plan.far
    orders, counts = [], []
    for z in range(far):
        here, order, count = set(), [], []
        for k in range(far):
            here.add(z ^ k)
            for plane in range(far):
                for half in range(2):
                    ready = plane in here and (half or plane == 0 or plane - 1 in here)
                    if ready and 2 * plane + half not in order:
                        order.append(2 * plane + half)
            count.append(len(order))
        orders.append(order)
        counts.append(count)
    return orders, [min(c[k] for c in counts) for k in range(far)]


def gather_and_compute(plan, own, every, sems, prepared, compute):
    send_sems, recv_sems = sems
    cuts, far = plan.cuts, plan.far
    t, c = lax.axis_index("tm"), lax.axis_index("dop")
    z, near = t // 4, t % 4
    beside = [flipped_by(near, k) for k in (1, 2, 3)]
    levels = [flipped_by(z, k) for k in range(far)]
    fellows = [flipped_by(c, k) for k in range(1, cuts)]

    partners = [(z * 4 + n, c) for n in beside]
    partners += [(other * 4 + near, c) for other in levels[1:]]
    partners += [(t, fellow) for fellow in fellows]
    barrier = pltpu.get_barrier_semaphore()
    for to, cut in partners:
        pl.semaphore_signal(
            barrier, inc=1, device_id={"tm": to, "dop": cut}, device_id_type=MESH
        )
    pl.semaphore_wait(barrier, len(partners))

    sent = []
    rows = own[0].shape[0]
    pad = (0, ROWS)

    def place(which, source):
        start = pl.multiple_of(source * rows, rows) + pad[which]
        return every[which].at[pl.ds(pl.multiple_of(start, 16), rows)]

    def copy(which, source, src, to, cut, slot):
        return pltpu.make_async_remote_copy(
            src_ref=src,
            dst_ref=place(which, source),
            send_sem=send_sems.at[slot],
            recv_sem=recv_sems.at[which, source],
            device_id={"tm": to, "dop": cut},
            device_id_type=MESH,
        )

    def send(source, to, cut, mine=False):
        for which in range(2):
            src = own[which] if mine else place(which, source)
            one = copy(which, source, src, to, cut, len(sent))
            one.start()
            sent.append(one)

    def landed(source):
        for which in range(2):
            copy(which, source, own[which], t, c, 0).wait_recv()

    def pass_on(k):
        for n in beside:
            source = (levels[k] * 4 + n) * cuts + c
            landed(source)
            for fellow in fellows:
                send(source, t, fellow)

    def complete(k):
        for fellow in fellows:
            for n in [near] + beside:
                landed((levels[k] * 4 + n) * cuts + fellow)

    me = t * cuts + c
    for level in levels[:0:-1]:
        send(me, level * 4 + near, c, True)
    for n in beside:
        send(me, z * 4 + n, c, True)
    for fellow in fellows:
        send(me, t, fellow, True)
    for which in range(2):
        every[which][pl.ds(pl.multiple_of(me * rows + pad[which], 16), rows)] = own[
            which
        ][...]
    prepared()

    pass_on(0)
    for level in levels[1:]:
        source = (level * 4 + near) * cuts + c
        landed(source)
        for n in beside:
            send(source, z * 4 + n, c)
        for fellow in fellows:
            send(source, t, fellow)
    orders, counts = schedule(plan)

    def group_at(i):
        group = orders[0][i] + 0 * z
        for other in range(1, far):
            group = jnp.where(z == other, orders[other][i], group)
        return group

    done = 0
    for k in range(far):
        complete(k)
        whole = [group_at(i) for i in range(done, counts[k])]
        if k == far - 1:
            compute(whole, done == 0, True)
            break
        for group in whole[:-1]:
            compute([group], done == 0, False)
            done += 1
        pass_on(k + 1)
        for group in whole[-1:]:
            compute([group], done == 0, False)
            done += 1
    return sent


def sends_needed(plan):
    far, fellows = plan.far, plan.cuts - 1
    return 2 * ((far - 1) + far * (3 + 4 * fellows))


def deal(plan, tiles, out, sems):
    send_sems, recv_sems = sems
    times = plan.times
    t, c = lax.axis_index("tm"), lax.axis_index("dop")
    me = t * plan.cuts + c
    fine = me // plan.share
    base = (me % plan.share) * plan.owners
    to_me = (base <= c) & (c < base + plan.owners)

    def copy(step, owner):
        to = flipped_by(t, step)
        return pltpu.make_async_remote_copy(
            src_ref=tiles.at[to * plan.lags // LANES, owner],
            dst_ref=out.at[fine],
            send_sem=send_sems.at[step, owner],
            recv_sem=recv_sems.at[fine],
            device_id={"tm": to, "dop": base + owner},
            device_id_type=MESH,
        )

    for step in range(times - 1, 0, -1):
        for owner in range(plan.owners):
            copy(step, owner).start()
    for owner in range(plan.owners):
        itself = base + owner == c

        @pl.when(jnp.logical_not(itself))
        def _():
            copy(0, owner).start()

        @pl.when(itself)
        def _():
            out[fine] = tiles[t * plan.lags // LANES, owner]

    for source in range(plan.fine):

        @pl.when((fine != source) | jnp.logical_not(to_me))
        def _():
            pltpu.make_async_remote_copy(
                src_ref=tiles.at[0, 0],
                dst_ref=out.at[source],
                send_sem=send_sems.at[0, 0],
                recv_sem=recv_sems.at[source],
                device_id={"tm": t, "dop": c},
                device_id_type=MESH,
            ).wait_recv()

    for step in range(1, times):
        for owner in range(plan.owners):
            copy(step, owner).wait_send()
    for owner in range(plan.owners):

        @pl.when(base + owner != c)
        def _():
            copy(0, owner).wait_send()


def whole_kernel(plan, s, r, waves_at, forward_at, back_at, out, *scratch):
    (gs, gr, waves, forward, back, tiles) = scratch[:6]
    drift, even, odd, held = scratch[6:10]
    stage, high, low, rstage, rhigh, rlow = scratch[10:16]
    S, R, yhigh, ylow, Z = scratch[16:21]
    load_sems, gather_sems, deal_sems = scratch[21], scratch[22:24], scratch[24:26]
    me = lax.axis_index("tm") * plan.cuts + lax.axis_index("dop")
    fine = me // plan.share
    first = (me % plan.share) * plan.mine
    loads = [
        pltpu.make_async_copy(source, target, load_sems.at[i])
        for i, (source, target) in enumerate(
            ((waves_at, waves), (forward_at, forward), (back_at, back))
        )
    ]

    def prepared():
        for load in loads:
            load.start()
        gr[:ROWS, :] = jnp.zeros((ROWS, LANES), jnp.bfloat16)
        prepare(plan, fine, drift, even, odd)
        for load in loads:
            load.wait()

    def compute(groups, start, last):
        for slot, group in enumerate(groups):
            work = (drift, even, odd, stage, high, low)
            signal_group(plan, group, slot, gs, waves, forward, work, S)
            reference_group(
                plan, group, slot, gr, waves, forward, (rstage, rhigh, rlow), R
            )
        if last:
            last_spectra(plan, first, len(groups), S, R, held, yhigh, ylow)
        else:
            add_spectra(plan, first, len(groups), S, R, held, start)

    sent = gather_and_compute(plan, (s, r), (gs, gr), gather_sems, prepared, compute)
    to_lags(plan, waves, back, yhigh, ylow, Z, tiles)
    deal(plan, tiles, out, deal_sems)
    for one in sent:
        one.wait_send()


def dealt_maps(plan, s, r):
    waves, forward, back = tables(plan)
    tall = plan.owners * SUB
    f32, bf16 = jnp.float32, jnp.bfloat16
    samples = 2 * plan.window // LANES
    counts = schedule(plan)[1]
    slots = counts[-1] - counts[-2]
    return pl.pallas_call(
        functools.partial(whole_kernel, plan),
        out_shape=jax.ShapeDtypeStruct((plan.fine, 2 * SUB, LANES), bf16),
        in_specs=[pl.BlockSpec(memory_space=pltpu.VMEM)] * 2
        + [pl.BlockSpec(memory_space=pl.ANY)] * 3,
        out_specs=pl.BlockSpec(memory_space=pltpu.VMEM),
        scratch_shapes=[
            pltpu.VMEM((samples, LANES), bf16),
            pltpu.VMEM((samples + ROWS, LANES), bf16),
            pltpu.VMEM(waves.shape, bf16),
            pltpu.VMEM(forward.shape, f32),
            pltpu.VMEM(back.shape, f32),
            pltpu.VMEM((N1, plan.owners, 2 * SUB, LANES), bf16),
            pltpu.VMEM((plan.groups, 2, SUB, LANES), f32),
            pltpu.VMEM((N1, 2, SUB, LANES), f32),
            pltpu.VMEM((N1, 2, SUB, LANES), f32),
            pltpu.VMEM((F1, plan.mine, 2, SUB, LANES), f32),
            pltpu.VMEM((SUB * APART + 7, LANES), f32),
            pltpu.VMEM((F1 * SUB, 2 * LANES), bf16),
            pltpu.VMEM((F1 * SUB, 2 * LANES), bf16),
            pltpu.VMEM((SUB * APART + APART + 7, LANES), f32),
            pltpu.VMEM((F1 * SUB, 2 * LANES), bf16),
            pltpu.VMEM((F1 * SUB, 2 * LANES), bf16),
            pltpu.VMEM((slots, F1 + plan.shifts, 2, SUB, LANES), f32),
            pltpu.VMEM((slots, F1, 2, SUB, LANES), f32),
            pltpu.VMEM((F1 * tall, 2 * LANES), bf16),
            pltpu.VMEM((F1 * tall, 2 * LANES), bf16),
            pltpu.VMEM((F1 * tall, 2 * LANES), f32),
            pltpu.SemaphoreType.DMA((3,)),
            pltpu.SemaphoreType.DMA((sends_needed(plan),)),
            pltpu.SemaphoreType.DMA((2, plan.devices)),
            pltpu.SemaphoreType.DMA((plan.times, plan.owners)),
            pltpu.SemaphoreType.DMA((plan.fine,)),
        ],
        compiler_params=pltpu.CompilerParams(
            collective_id=0,
            has_side_effects=True,
            vmem_limit_bytes=56 * 1024 * 1024,
        ),
    )(s, r, jnp.asarray(waves), jnp.asarray(forward), jnp.asarray(back))


def flipped(index, bit):
    weight = 1 << bit
    return index + weight * (1 - 2 * ((index // weight) % 2))


def flipped_by(index, mask):
    for bit in range(mask.bit_length()):
        if mask >> bit & 1:
            index = flipped(index, bit)
    return index


def order_of(plan):
    bins = F // plan.cuts
    order = np.zeros((plan.fine, 2, SUB, 2, bins), np.float32)
    for fine in range(plan.fine):
        for part in range(2):
            for i in range(plan.per_owner):
                order[fine, part, i, part, plan.fine * i + fine] = 1.0
    return order.reshape(plan.fine * 2 * SUB, 2 * bins).astype(jnp.bfloat16)


def settle_kernel(plan, tiles, order, out):
    rows = plan.fine * 2 * SUB
    wide = lax.dot_general(
        tiles[...].reshape(rows, LANES),
        order[...],
        (((0,), (0,)), ((), ())),
        preferred_element_type=jnp.float32,
    )
    bins = F // plan.cuts
    if plan.lags < LANES:
        pieces = LANES // plan.lags
        which = lax.axis_index("tm") % pieces
        kept = wide[: plan.lags]
        for piece in range(1, pieces):
            kept = jnp.where(
                which == piece, wide[piece * plan.lags : (piece + 1) * plan.lags], kept
            )
        wide = kept
    out[:, 0, :] = wide[:, :bins]
    out[:, 1, :] = wide[:, bins:]


def settled(plan, tiles):
    return pl.pallas_call(
        functools.partial(settle_kernel, plan),
        out_shape=jax.ShapeDtypeStruct((plan.lags, 2, F // plan.cuts), jnp.float32),
        in_specs=[pl.BlockSpec(memory_space=pltpu.VMEM)] * 2,
        out_specs=pl.BlockSpec(memory_space=pltpu.VMEM),
    )(tiles, jnp.asarray(order_of(plan)))


def paired_rows(x):
    samples = x.shape[1] * x.shape[2]
    split = x.reshape(2, samples // LANES, LANES).transpose(1, 0, 2)
    return split.reshape(2 * samples // LANES, LANES)


def on_device(surveillance, reference_signal):
    times, cuts = lax.axis_size("tm"), lax.axis_size("dop")
    samples = surveillance.shape[1] * surveillance.shape[2]
    plan = Plan(times, cuts, samples * times * cuts)
    tiles = dealt_maps(plan, paired_rows(surveillance), paired_rows(reference_signal))
    return settled(plan, tiles)


def solution(mesh):
    return jax.shard_map(
        on_device,
        mesh=mesh,
        in_specs=(P(None, "tm", "dop"), P(None, "tm", "dop")),
        out_specs=P("tm", None, "dop"),
        check_vma=False,
    )
```

```python
import functools
import math

import jax
import jax.numpy as jnp
import numpy as np
from jax import lax
from jax.experimental import pallas as pl
from jax.experimental.pallas import tpu as pltpu
from jax.sharding import PartitionSpec as P

F = 512
LAGS = 2048
LANES = 128
SUB = 8
POINTS = 2 * LAGS
N1 = LAGS // LANES
F1 = POINTS // LANES
ROWS = 2 * N1
GROUP = SUB * ROWS
APART = ROWS + 1
MESH = pl.DeviceIdType.MESH
SIGNAL, REFER, HELD = 0, 6, 12


class Plan:
    def __init__(self, times, cuts, window):
        self.times, self.cuts, self.window = times, cuts, window
        self.devices = times * cuts
        self.groups = window // (SUB * LAGS)
        self.far = times // 4
        self.fine = window // POINTS
        self.shifts = F // self.fine
        self.share = self.devices // self.fine
        self.mine = self.shifts // self.share
        self.per_owner = self.shifts // cuts
        self.owners = self.mine // self.per_owner
        self.lags = LAGS // times


def halves(x):
    high = x.astype(jnp.bfloat16)
    low = (x - high.astype(jnp.float32)).astype(jnp.bfloat16)
    return high, low


def tables(plan):
    a = np.arange(LANES)
    angle = 2.0 * np.pi / LANES * np.mod(a[:, None] * a[None, :], LANES)
    c, s = np.cos(angle), np.sin(angle)
    waves = []
    for sign in (-1.0, 1.0):
        full = np.block([[c, sign * s], [-sign * s, c]])
        high = full.astype(jnp.bfloat16)
        low = (full - high.astype(np.float64)).astype(jnp.bfloat16)
        waves += [high, low]
    turn = 2.0 * np.pi / POINTS * np.arange(F1)[:, None] * a[None, :]
    turns = np.stack([np.cos(turn), -np.sin(turn)], 1)
    sign = np.where(
        (np.arange(F1)[:, None] * np.arange(SUB)[None, :]) % 2 == 1, -1.0, 1.0
    )
    forward = (turns[:, :, None, :] * sign[:, None, :, None]).astype(np.float32)
    scale = 1.0 / (POINTS * math.sqrt(plan.window))
    back = (np.stack([np.cos(turn), np.sin(turn)], 1) * scale).astype(np.float32)
    back = np.broadcast_to(back[:, :, None, :], (F1, 2, SUB, LANES)).copy()
    return np.stack(waves), forward, back


def times_(x, y):
    return x[0] * y[0] - x[1] * y[1], x[0] * y[1] + x[1] * y[0]


def plus(x, y):
    return x[0] + y[0], x[1] + y[1]


def minus(x, y):
    return x[0] - y[0], x[1] - y[1]


def turned(x, numerator, denominator, sign):
    eighth = (8 * numerator) % (8 * denominator) / denominator
    if eighth == 0:
        return x
    if eighth == 4:
        return -x[0], -x[1]
    if eighth in (2, 6):
        if (eighth == 2) == (sign > 0):
            return -x[1], x[0]
        return x[1], -x[0]
    angle = 2.0 * math.pi * numerator / denominator
    c, s = math.cos(angle), sign * math.sin(angle)
    return x[0] * c - x[1] * s, x[1] * c + x[0] * s


def dft4(x, sign):
    a, b = plus(x[0], x[2]), minus(x[0], x[2])
    c, d = plus(x[1], x[3]), turned(minus(x[1], x[3]), 1, 4, sign)
    return [plus(a, c), plus(b, d), minus(a, c), minus(b, d)]


def dft16(x, sign):
    inner = [dft4(x[i::4], sign) for i in range(4)]
    out = [None] * 16
    for k in range(4):
        column = [turned(inner[i][k], i * k, 16, sign) for i in range(4)]
        for j, value in enumerate(dft4(column, sign)):
            out[k + 4 * j] = value
    return out


def phases_of(steps, window):
    angle = lax.bitwise_and(steps, window - 1).astype(jnp.float32) * (
        2.0 * math.pi / window
    )
    return jnp.cos(angle), -jnp.sin(angle)


def prepare(plan, fine, drift, even, odd):
    sub = lax.broadcasted_iota(jnp.int32, (SUB, LANES), 0)
    lane = lax.broadcasted_iota(jnp.int32, (SUB, LANES), 1)

    @pl.loop(0, plan.groups)
    def _(group):
        segment = SUB * group + sub
        c, s = phases_of(fine * (lane + segment * LAGS), plan.window)
        drift[group, 0] = c
        drift[group, 1] = s

    @pl.loop(0, N1)
    def _(row):
        steps = jnp.full((SUB, LANES), fine * LANES * row, jnp.int32)
        c, s = phases_of(steps, plan.window)
        even[row, 0] = c
        even[row, 1] = s
        c, s = phases_of(steps + row * (plan.window // F1), plan.window)
        odd[row, 0] = c
        odd[row, 1] = s


def staged(rows, stage, skip=0):
    for i in range(rows.shape[0] // ROWS):
        at = (i + skip) * APART
        stage[at : at + ROWS, :] = rows[i * ROWS : (i + 1) * ROWS, :].astype(jnp.float32)


def spread_rows(stage, skip=0):
    first = skip * APART
    return [
        tuple(
            stage[pl.ds(first + 2 * n + part, SUB, stride=APART), :]
            for part in range(2)
        )
        for n in range(N1)
    ]


def turn_and_split(found, parity, forward, high, low):
    for pair in range(N1 // 2):
        both = []
        for e in (2 * pair, 2 * pair + 1):
            f1 = 2 * e + parity
            both.append(times_(found[e], (forward[f1, 0], forward[f1, 1])))
        rows = slice(parity * 128 + pair * 16, parity * 128 + pair * 16 + 16)
        for part in range(2):
            h, l = halves(jnp.concatenate([both[0][part], both[1][part]], 0))
            lanes = slice(part * LANES, (part + 1) * LANES)
            high[rows, lanes] = h
            low[rows, lanes] = l


def lanes_turned(high, low, waves, at):
    return (
        jnp.dot(high[...], waves[at], preferred_element_type=jnp.float32)
        + jnp.dot(low[...], waves[at], preferred_element_type=jnp.float32)
        + jnp.dot(high[...], waves[at + 1], preferred_element_type=jnp.float32)
    )


def signal_group(plan, group, slot, gs, waves, forward, work, A):
    drift, even, odd, stage, high, low = work
    stage, high, low = stage.at[slot], high.at[slot], low.at[slot]
    start = pl.multiple_of(group * GROUP, GROUP)
    staged(gs[pl.ds(start, GROUP), :], stage)
    here = (drift[group, 0], drift[group, 1])
    x = [times_(v, here) for v in spread_rows(stage)]
    for parity, table in enumerate((even, odd)):
        y = [times_(x[n], (table[n, 0], table[n, 1])) for n in range(N1)]
        turn_and_split(dft16(y, -1), parity, forward, high, low)
    wide = lanes_turned(high, low, waves, 0)
    reach = plan.shifts // 2
    for f1 in range(F1):
        row = (f1 % 2) * 128 + (f1 // 2) * SUB
        re = wide[row : row + SUB, :LANES]
        im = wide[row : row + SUB, LANES:]
        for k, v in enumerate((re + im, re, im)):
            A[reach + f1, SIGNAL + 3 * slot + k] = v
            if f1 < reach:
                A[reach + f1 + F1, SIGNAL + 3 * slot + k] = pltpu.roll(
                    v, LANES - 1, 1
                )
            if f1 >= F1 - reach:
                A[reach + f1 - F1, SIGNAL + 3 * slot + k] = pltpu.roll(v, 1, 1)


def reference_group(plan, group, slot, gr, before, waves, forward, work, A):
    stage, high, low = work
    stage, high, low = stage.at[slot], high.at[slot], low.at[slot]
    start = pl.multiple_of(group * GROUP, GROUP)
    if before is None:
        staged(gr[pl.ds(start, GROUP + ROWS), :], stage)
    else:
        staged(before[...], stage)
        own = pl.multiple_of(start + ROWS, ROWS)
        staged(gr[pl.ds(own, GROUP), :], stage, 1)
    before, now = spread_rows(stage), spread_rows(stage, 1)
    y = [plus(a, b) for a, b in zip(now, before)]
    turn_and_split(dft16(y, -1), 0, forward, high, low)
    y = [turned(minus(a, b), n, F1, -1) for n, (a, b) in enumerate(zip(now, before))]
    turn_and_split(dft16(y, -1), 1, forward, high, low)
    wide = lanes_turned(high, low, waves, 0)
    for f1 in range(F1):
        row = (f1 % 2) * 128 + (f1 // 2) * SUB
        re = wide[row : row + SUB, :LANES]
        im = wide[row : row + SUB, LANES:]
        for k, v in enumerate((re, re + im, re - im)):
            A[f1, REFER + 3 * slot + k] = v


def product(plan, first, f1, index, slots, A, start):
    at = f1 + first + index
    sums = [None] * 3 if start else [A[f1, HELD + 3 * index + k] for k in range(3)]
    for slot in range(slots):
        for k in range(3):
            v = A[at, SIGNAL + 3 * slot + k] * A[f1, REFER + 3 * slot + k]
            sums[k] = v if sums[k] is None else sums[k] + v
    return sums


def add_spectra(plan, first, slots, A, start):
    step = 4

    @pl.loop(0, F1 // step)
    def _(block):
        for k in range(step):
            f1 = block * step + k
            for index in range(plan.mine):
                sums = product(plan, first, f1, index, slots, A, start)
                for which in range(3):
                    A[f1, HELD + 3 * index + which] = sums[which]


def last_spectra(plan, first, slots, A, fold, high, low):
    step = 2
    tall = plan.owners * SUB

    @pl.loop(0, F1 // step)
    def _(block):
        for k in range(step):
            f1 = block * step + k
            for index in range(plan.mine):
                one, two, three = product(plan, first, f1, index, slots, A, False)
                row = index // plan.per_owner * SUB + index % plan.per_owner
                at = row * (SUB + 1)
                fold[k, 0, at : at + SUB, :] = one - three
                fold[k, 1, at : at + SUB, :] = one - two
            rows = pl.ds(pl.multiple_of(f1 * tall, tall), tall)
            for part in range(2):
                found = []
                for owner in range(plan.owners):
                    at = owner * SUB * (SUB + 1)
                    parts = [
                        fold[k, part, pl.ds(at + i, SUB, stride=SUB + 1), :]
                        for i in range(SUB)
                    ]
                    while len(parts) > 1:
                        parts = [x + y for x, y in zip(parts[::2], parts[1::2])]
                    found.append(parts[0])
                h, l = halves(jnp.concatenate(found, 0))
                lanes = slice(part * LANES, (part + 1) * LANES)
                high[rows, lanes] = h
                low[rows, lanes] = l


def to_lags(plan, waves, back, high, low, Z, out):
    Z[...] = lanes_turned(high, low, waves, 2)
    tall = plan.owners * SUB
    for owner in range(plan.owners):
        z = []
        for f1 in range(F1):
            rows = slice(f1 * tall + owner * SUB, f1 * tall + owner * SUB + SUB)
            v = (Z[rows, :LANES], Z[rows, LANES:])
            z.append(times_(v, (back[f1, 0], back[f1, 1])))
        half = F1 // 2
        sums = dft16([plus(z[i], z[i + half]) for i in range(half)], 1)
        gaps = dft16(
            [turned(minus(z[i], z[i + half]), i, F1, 1) for i in range(half)], 1
        )
        for e in range(N1 // 2):
            for parity, found in enumerate((sums, gaps)):
                out[2 * e + parity, owner] = jnp.concatenate(found[e], 0).astype(
                    jnp.bfloat16
                )


def gather_and_compute(plan, own, every, ahead, sems, prepared, transform, add):
    send_sems, recv_sems, ahead_send, ahead_recv = sems
    cuts, far = plan.cuts, plan.far
    t, c = lax.axis_index("tm"), lax.axis_index("dop")
    z, near = t // 4, t % 4
    beside = [flipped_by(near, k) for k in (1, 2, 3)]
    levels = [z] + [k + (k + far - z) // far for k in range(far - 1)]
    fellows = [flipped_by(c, k) for k in range(1, cuts)]

    partners = [(z * 4 + n, c) for n in beside]
    partners += [(other * 4 + near, c) for other in levels[1:]]
    partners += [(t, fellow) for fellow in fellows]
    barrier = pltpu.get_barrier_semaphore()
    for to, cut in partners:
        pl.semaphore_signal(
            barrier, inc=1, device_id={"tm": to, "dop": cut}, device_id_type=MESH
        )
    rows = own[0].shape[0]
    tail = min(rows, ROWS)
    enders = ROWS // tail
    ends = (near == 3) & (c >= cuts - enders) & (z < far - 1)

    @pl.when(z > 0)
    def _():
        for i in range(enders):
            pl.semaphore_signal(
                barrier,
                inc=1,
                device_id={"tm": t - near - 1, "dop": cuts - enders + i},
                device_id_type=MESH,
            )

    pl.semaphore_wait(barrier, len(partners) + jnp.where(ends, 4 * cuts, 0))

    def forerun(slot, n, cut):
        which = jnp.maximum(c - (cuts - enders), 0)
        return pltpu.make_async_remote_copy(
            src_ref=own[1].at[pl.ds(rows - tail, tail)],
            dst_ref=ahead.at[pl.ds(pl.multiple_of(which * tail, tail), tail)],
            send_sem=ahead_send.at[slot],
            recv_sem=ahead_recv.at[which],
            device_id={"tm": jnp.minimum(z + 1, far - 1) * 4 + n, "dop": cut},
            device_id_type=MESH,
        )

    spots = [(n, cut) for n in range(4) for cut in range(cuts)]

    @pl.when(ends)
    def _():
        for slot, (n, cut) in enumerate(spots):
            forerun(slot, n, cut).start()

    sent = []
    pad = (0, ROWS)

    def place(which, source):
        start = pl.multiple_of(source * rows, rows) + pad[which]
        return every[which].at[pl.ds(pl.multiple_of(start, 16), rows)]

    def copy(which, source, src, to, cut, slot):
        return pltpu.make_async_remote_copy(
            src_ref=src,
            dst_ref=place(which, source),
            send_sem=send_sems.at[slot],
            recv_sem=recv_sems.at[which, source],
            device_id={"tm": to, "dop": cut},
            device_id_type=MESH,
        )

    def send(source, to, cut, mine=False):
        for which in range(2):
            src = own[which] if mine else place(which, source)
            one = copy(which, source, src, to, cut, len(sent))
            one.start()
            sent.append(one)

    def landed(source):
        for which in range(2):
            copy(which, source, own[which], t, c, 0).wait_recv()

    def pass_on(k):
        for n in beside:
            source = (levels[k] * 4 + n) * cuts + c
            landed(source)
            for fellow in fellows:
                send(source, t, fellow)

    def complete(k):
        for fellow in fellows:
            for n in [near] + beside:
                landed((levels[k] * 4 + n) * cuts + fellow)

    me = t * cuts + c
    for level in levels[1:]:
        send(me, level * 4 + near, c, True)
    for n in beside:
        send(me, z * 4 + n, c, True)
    for fellow in fellows:
        send(me, t, fellow, True)
    for which in range(2):
        every[which][pl.ds(pl.multiple_of(me * rows + pad[which], 16), rows)] = own[
            which
        ][...]
    prepared()

    pass_on(0)
    for level in levels[1:]:
        source = (level * 4 + near) * cuts + c
        landed(source)
        for n in beside:
            send(source, z * 4 + n, c)
        for fellow in fellows:
            send(source, t, fellow)

    @pl.when(z == 0)
    def _():
        ahead[...] = jnp.zeros((ROWS, LANES), jnp.bfloat16)

    @pl.when(z > 0)
    def _():
        for i in range(enders):
            pltpu.make_async_remote_copy(
                src_ref=own[1].at[pl.ds(rows - tail, tail)],
                dst_ref=ahead.at[pl.ds(i * tail, tail)],
                send_sem=ahead_send.at[0],
                recv_sem=ahead_recv.at[i],
                device_id={"tm": t, "dop": c},
                device_id_type=MESH,
            ).wait_recv()

    for k in range(far):
        complete(k)
        transform([2 * levels[k], 2 * levels[k] + 1], ahead if k == 0 else None)
        if k < far - 1:
            pass_on(k + 1)
        add(k == 0, k == far - 1)

    @pl.when(ends)
    def _():
        for slot, (n, cut) in enumerate(spots):
            forerun(slot, n, cut).wait_send()

    return sent


def sends_needed(plan):
    far, fellows = plan.far, plan.cuts - 1
    return 2 * ((far - 1) + far * (3 + 4 * fellows))


def deal(plan, tiles, out, sems):
    send_sems, recv_sems = sems
    times = plan.times
    t, c = lax.axis_index("tm"), lax.axis_index("dop")
    me = t * plan.cuts + c
    fine = me // plan.share
    base = (me % plan.share) * plan.owners
    to_me = (base <= c) & (c < base + plan.owners)

    def copy(step, owner):
        to = flipped_by(t, step)
        return pltpu.make_async_remote_copy(
            src_ref=tiles.at[to * plan.lags // LANES, owner],
            dst_ref=out.at[fine],
            send_sem=send_sems.at[step, owner],
            recv_sem=recv_sems.at[fine],
            device_id={"tm": to, "dop": base + owner},
            device_id_type=MESH,
        )

    for step in range(times - 1, 0, -1):
        for owner in range(plan.owners):
            copy(step, owner).start()
    for owner in range(plan.owners):
        itself = base + owner == c

        @pl.when(jnp.logical_not(itself))
        def _():
            copy(0, owner).start()

        @pl.when(itself)
        def _():
            out[fine] = tiles[t * plan.lags // LANES, owner]

    for source in range(plan.fine):

        @pl.when((fine != source) | jnp.logical_not(to_me))
        def _():
            pltpu.make_async_remote_copy(
                src_ref=tiles.at[0, 0],
                dst_ref=out.at[source],
                send_sem=send_sems.at[0, 0],
                recv_sem=recv_sems.at[source],
                device_id={"tm": t, "dop": c},
                device_id_type=MESH,
            ).wait_recv()

    for step in range(1, times):
        for owner in range(plan.owners):
            copy(step, owner).wait_send()
    for owner in range(plan.owners):

        @pl.when(base + owner != c)
        def _():
            copy(0, owner).wait_send()


def whole_kernel(plan, s, r, waves_at, forward_at, back_at, out, *scratch):
    (gs, gr, waves, forward, back, tiles) = scratch[:6]
    drift, even, odd, A, ahead, fold = scratch[6:12]
    stage, high, low, rstage, rhigh, rlow = scratch[12:18]
    yhigh, ylow, Z = scratch[18:21]
    load_sems, gather_sems, deal_sems = scratch[21], scratch[22:26], scratch[26:28]
    me = lax.axis_index("tm") * plan.cuts + lax.axis_index("dop")
    fine = me // plan.share
    first = 0 if plan.share == 1 else (me % plan.share) * plan.mine
    loads = [
        pltpu.make_async_copy(source, target, load_sems.at[i])
        for i, (source, target) in enumerate(
            ((waves_at, waves), (forward_at, forward), (back_at, back))
        )
    ]

    def prepared():
        for load in loads:
            load.start()
        gr[:ROWS, :] = jnp.zeros((ROWS, LANES), jnp.bfloat16)
        prepare(plan, fine, drift, even, odd)
        for load in loads:
            load.wait()

    def transform(groups, before):
        for slot, group in enumerate(groups):
            work = (drift, even, odd, stage, high, low)
            signal_group(plan, group, slot, gs, waves, forward, work, A)
            work = (rstage, rhigh, rlow)
            head = before if slot == 0 else None
            reference_group(plan, group, slot, gr, head, waves, forward, work, A)

    def add(start, last):
        if last:
            last_spectra(plan, first, 2, A, fold, yhigh, ylow)
        else:
            add_spectra(plan, first, 2, A, start)

    sent = gather_and_compute(
        plan, (s, r), (gs, gr), ahead, gather_sems, prepared, transform, add
    )
    to_lags(plan, waves, back, yhigh, ylow, Z, tiles)
    deal(plan, tiles, out, deal_sems)
    for one in sent:
        one.wait_send()


def dealt_maps(plan, s, r):
    waves, forward, back = tables(plan)
    tall = plan.owners * SUB
    f32, bf16 = jnp.float32, jnp.bfloat16
    samples = 2 * plan.window // LANES
    slots = 2
    width = -(-(HELD + 3 * plan.mine) // 4) * 4
    enders = max(1, ROWS * plan.devices // samples)
    return pl.pallas_call(
        functools.partial(whole_kernel, plan),
        out_shape=jax.ShapeDtypeStruct((plan.fine, 2 * SUB, LANES), bf16),
        in_specs=[pl.BlockSpec(memory_space=pltpu.VMEM)] * 2
        + [pl.BlockSpec(memory_space=pl.ANY)] * 3,
        out_specs=pl.BlockSpec(memory_space=pltpu.VMEM),
        scratch_shapes=[
            pltpu.VMEM((samples, LANES), bf16),
            pltpu.VMEM((samples + ROWS, LANES), bf16),
            pltpu.VMEM(waves.shape, bf16),
            pltpu.VMEM(forward.shape, f32),
            pltpu.VMEM(back.shape, f32),
            pltpu.VMEM((N1, plan.owners, 2 * SUB, LANES), bf16),
            pltpu.VMEM((plan.groups, 2, SUB, LANES), f32),
            pltpu.VMEM((N1, 2, SUB, LANES), f32),
            pltpu.VMEM((N1, 2, SUB, LANES), f32),
            pltpu.VMEM((F1 + plan.shifts, width, SUB, LANES), f32),
            pltpu.VMEM((ROWS, LANES), bf16),
            pltpu.VMEM((2, 2, tall * (SUB + 1) + 7, LANES), f32),
            pltpu.VMEM((slots, SUB * APART + 7, LANES), f32),
            pltpu.VMEM((slots, F1 * SUB, 2 * LANES), bf16),
            pltpu.VMEM((slots, F1 * SUB, 2 * LANES), bf16),
            pltpu.VMEM((slots, SUB * APART + APART + 7, LANES), f32),
            pltpu.VMEM((slots, F1 * SUB, 2 * LANES), bf16),
            pltpu.VMEM((slots, F1 * SUB, 2 * LANES), bf16),
            pltpu.VMEM((F1 * tall, 2 * LANES), bf16),
            pltpu.VMEM((F1 * tall, 2 * LANES), bf16),
            pltpu.VMEM((F1 * tall, 2 * LANES), f32),
            pltpu.SemaphoreType.DMA((3,)),
            pltpu.SemaphoreType.DMA((sends_needed(plan),)),
            pltpu.SemaphoreType.DMA((2, plan.devices)),
            pltpu.SemaphoreType.DMA((4 * plan.cuts,)),
            pltpu.SemaphoreType.DMA((enders,)),
            pltpu.SemaphoreType.DMA((plan.times, plan.owners)),
            pltpu.SemaphoreType.DMA((plan.fine,)),
        ],
        compiler_params=pltpu.CompilerParams(
            collective_id=0,
            has_side_effects=True,
            vmem_limit_bytes=56 * 1024 * 1024,
        ),
    )(s, r, jnp.asarray(waves), jnp.asarray(forward), jnp.asarray(back))


def flipped(index, bit):
    weight = 1 << bit
    return index + weight * (1 - 2 * ((index // weight) % 2))


def flipped_by(index, mask):
    for bit in range(mask.bit_length()):
        if mask >> bit & 1:
            index = flipped(index, bit)
    return index


def order_of(plan):
    bins = F // plan.cuts
    order = np.zeros((plan.fine, 2, SUB, 2, bins), np.float32)
    for fine in range(plan.fine):
        for part in range(2):
            for i in range(plan.per_owner):
                order[fine, part, i, part, plan.fine * i + fine] = 1.0
    return order.reshape(plan.fine * 2 * SUB, 2 * bins).astype(jnp.bfloat16)


def settle_kernel(plan, tiles, order, out):
    rows = plan.fine * 2 * SUB
    wide = lax.dot_general(
        tiles[...].reshape(rows, LANES),
        order[...],
        (((0,), (0,)), ((), ())),
        preferred_element_type=jnp.float32,
    )
    bins = F // plan.cuts
    if plan.lags < LANES:
        pieces = LANES // plan.lags
        which = lax.axis_index("tm") % pieces
        kept = wide[: plan.lags]
        for piece in range(1, pieces):
            kept = jnp.where(
                which == piece, wide[piece * plan.lags : (piece + 1) * plan.lags], kept
            )
        wide = kept
    out[:, 0, :] = wide[:, :bins]
    out[:, 1, :] = wide[:, bins:]


def settled(plan, tiles):
    return pl.pallas_call(
        functools.partial(settle_kernel, plan),
        out_shape=jax.ShapeDtypeStruct((plan.lags, 2, F // plan.cuts), jnp.float32),
        in_specs=[pl.BlockSpec(memory_space=pltpu.VMEM)] * 2,
        out_specs=pl.BlockSpec(memory_space=pltpu.VMEM),
    )(tiles, jnp.asarray(order_of(plan)))


def paired_rows(x):
    samples = x.shape[1] * x.shape[2]
    split = x.reshape(2, samples // LANES, LANES).transpose(1, 0, 2)
    return split.reshape(2 * samples // LANES, LANES)


def on_device(surveillance, reference_signal):
    times, cuts = lax.axis_size("tm"), lax.axis_size("dop")
    samples = surveillance.shape[1] * surveillance.shape[2]
    plan = Plan(times, cuts, samples * times * cuts)
    tiles = dealt_maps(plan, paired_rows(surveillance), paired_rows(reference_signal))
    return settled(plan, tiles)


def solution(mesh):
    return jax.shard_map(
        on_device,
        mesh=mesh,
        in_specs=(P(None, "tm", "dop"), P(None, "tm", "dop")),
        out_specs=P("tm", None, "dop"),
        check_vma=False,
    )
```

```python
import functools
import math

import jax
import jax.numpy as jnp
import numpy as np
from jax import lax
from jax.experimental import pallas as pl
from jax.experimental.pallas import tpu as pltpu
from jax.sharding import PartitionSpec as P

F = 512
LAGS = 2048
LANES = 128
SUB = 8
POINTS = 2 * LAGS
N1 = LAGS // LANES
F1 = POINTS // LANES
ROWS = 2 * N1
GROUP = SUB * ROWS
APART = ROWS + 1
MESH = pl.DeviceIdType.MESH
SIGNAL, REFER, HELD = 0, 6, 12


class Plan:
    def __init__(self, times, cuts, window):
        self.times, self.cuts, self.window = times, cuts, window
        self.devices = times * cuts
        self.groups = window // (SUB * LAGS)
        self.far = times // 4
        self.fine = window // POINTS
        self.shifts = F // self.fine
        self.share = self.devices // self.fine
        self.mine = self.shifts // self.share
        self.per_owner = self.shifts // cuts
        self.owners = self.mine // self.per_owner
        self.lags = LAGS // times


def halves(x):
    high = x.astype(jnp.bfloat16)
    low = (x - high.astype(jnp.float32)).astype(jnp.bfloat16)
    return high, low


def tables(plan):
    a = np.arange(LANES)
    angle = 2.0 * np.pi / LANES * np.mod(a[:, None] * a[None, :], LANES)
    c, s = np.cos(angle), np.sin(angle)
    waves = []
    for sign in (-1.0, 1.0):
        full = np.block([[c, sign * s], [-sign * s, c]])
        high = full.astype(jnp.bfloat16)
        low = (full - high.astype(np.float64)).astype(jnp.bfloat16)
        waves += [high, low]
    turn = 2.0 * np.pi / POINTS * np.arange(F1)[:, None] * a[None, :]
    turns = np.stack([np.cos(turn), -np.sin(turn)], 1)
    sign = np.where(
        (np.arange(F1)[:, None] * np.arange(SUB)[None, :]) % 2 == 1, -1.0, 1.0
    )
    forward = (turns[:, :, None, :] * sign[:, None, :, None]).astype(np.float32)
    scale = 1.0 / (POINTS * math.sqrt(plan.window))
    back = (np.stack([np.cos(turn), np.sin(turn)], 1) * scale).astype(np.float32)
    back = np.broadcast_to(back[:, :, None, :], (F1, 2, SUB, LANES)).copy()
    return np.stack(waves), forward, back


def times_(x, y):
    return x[0] * y[0] - x[1] * y[1], x[0] * y[1] + x[1] * y[0]


def plus(x, y):
    return x[0] + y[0], x[1] + y[1]


def minus(x, y):
    return x[0] - y[0], x[1] - y[1]


def turned(x, numerator, denominator, sign):
    eighth = (8 * numerator) % (8 * denominator) / denominator
    if eighth == 0:
        return x
    if eighth == 4:
        return -x[0], -x[1]
    if eighth in (2, 6):
        if (eighth == 2) == (sign > 0):
            return -x[1], x[0]
        return x[1], -x[0]
    angle = 2.0 * math.pi * numerator / denominator
    c, s = math.cos(angle), sign * math.sin(angle)
    return x[0] * c - x[1] * s, x[1] * c + x[0] * s


def dft4(x, sign):
    a, b = plus(x[0], x[2]), minus(x[0], x[2])
    c, d = plus(x[1], x[3]), turned(minus(x[1], x[3]), 1, 4, sign)
    return [plus(a, c), plus(b, d), minus(a, c), minus(b, d)]


def dft16(x, sign):
    inner = [dft4(x[i::4], sign) for i in range(4)]
    out = [None] * 16
    for k in range(4):
        column = [turned(inner[i][k], i * k, 16, sign) for i in range(4)]
        for j, value in enumerate(dft4(column, sign)):
            out[k + 4 * j] = value
    return out


def phases_of(steps, window):
    angle = lax.bitwise_and(steps, window - 1).astype(jnp.float32) * (
        2.0 * math.pi / window
    )
    return jnp.cos(angle), -jnp.sin(angle)


def prepare(plan, fine, drift, even, odd):
    sub = lax.broadcasted_iota(jnp.int32, (SUB, LANES), 0)
    lane = lax.broadcasted_iota(jnp.int32, (SUB, LANES), 1)

    @pl.loop(0, plan.groups)
    def _(group):
        segment = SUB * group + sub
        c, s = phases_of(fine * (lane + segment * LAGS), plan.window)
        drift[group, 0] = c
        drift[group, 1] = s

    @pl.loop(0, N1)
    def _(row):
        steps = jnp.full((SUB, LANES), fine * LANES * row, jnp.int32)
        c, s = phases_of(steps, plan.window)
        even[row, 0] = c
        even[row, 1] = s
        c, s = phases_of(steps + row * (plan.window // F1), plan.window)
        odd[row, 0] = c
        odd[row, 1] = s


def staged(rows, stage, skip=0):
    for i in range(rows.shape[0] // ROWS):
        at = (i + skip) * APART
        stage[at : at + ROWS, :] = rows[i * ROWS : (i + 1) * ROWS, :].astype(jnp.float32)


def spread_rows(stage, skip=0):
    first = skip * APART
    return [
        tuple(
            stage[pl.ds(first + 2 * n + part, SUB, stride=APART), :]
            for part in range(2)
        )
        for n in range(N1)
    ]


def turn_and_split(found, parity, forward, high, low):
    for pair in range(N1 // 2):
        both = []
        for e in (2 * pair, 2 * pair + 1):
            f1 = 2 * e + parity
            both.append(times_(found[e], (forward[f1, 0], forward[f1, 1])))
        rows = slice(parity * 128 + pair * 16, parity * 128 + pair * 16 + 16)
        for part in range(2):
            h, l = halves(jnp.concatenate([both[0][part], both[1][part]], 0))
            lanes = slice(part * LANES, (part + 1) * LANES)
            high[rows, lanes] = h
            low[rows, lanes] = l


def lanes_turned(high, low, waves, at):
    return (
        jnp.dot(high[...], waves[at], preferred_element_type=jnp.float32)
        + jnp.dot(low[...], waves[at], preferred_element_type=jnp.float32)
        + jnp.dot(high[...], waves[at + 1], preferred_element_type=jnp.float32)
    )


def signal_rows(plan, group, slot, gs, forward, work):
    drift, even, odd, stage, high, low = work
    stage, high, low = stage.at[slot], high.at[slot, 0], low.at[slot, 0]
    start = pl.multiple_of(group * GROUP, GROUP)
    staged(gs[pl.ds(start, GROUP), :], stage)
    here = (drift[group, 0], drift[group, 1])
    x = [times_(v, here) for v in spread_rows(stage)]
    for parity, table in enumerate((even, odd)):
        y = [times_(x[n], (table[n, 0], table[n, 1])) for n in range(N1)]
        turn_and_split(dft16(y, -1), parity, forward, high, low)


def reference_rows(plan, group, slot, gr, before, forward, work):
    stage, high, low = work
    stage, high, low = stage.at[slot], high.at[slot, 1], low.at[slot, 1]
    start = pl.multiple_of(group * GROUP, GROUP)
    if before is None:
        staged(gr[pl.ds(start, GROUP + ROWS), :], stage)
    else:
        staged(before[...], stage)
        own = pl.multiple_of(start + ROWS, ROWS)
        staged(gr[pl.ds(own, GROUP), :], stage, 1)
    before, now = spread_rows(stage), spread_rows(stage, 1)
    y = [plus(a, b) for a, b in zip(now, before)]
    turn_and_split(dft16(y, -1), 0, forward, high, low)
    y = [turned(minus(a, b), n, F1, -1) for n, (a, b) in enumerate(zip(now, before))]
    turn_and_split(dft16(y, -1), 1, forward, high, low)


def group_spectra(plan, slot, waves, high, low, A):
    tall = F1 * SUB
    shape = (2 * tall, 2 * LANES)
    wide = lanes_turned(high[slot].reshape(shape), low[slot].reshape(shape), waves, 0)
    reach = plan.shifts // 2
    for f1 in range(F1):
        row = (f1 % 2) * 128 + (f1 // 2) * SUB
        re = wide[row : row + SUB, :LANES]
        im = wide[row : row + SUB, LANES:]
        for k, v in enumerate((re + im, re, im)):
            at = SIGNAL + 3 * slot + k
            A[reach + f1, at] = v
            if f1 < reach:
                A[reach + f1 + F1, at] = pltpu.roll(v, LANES - 1, 1)
            if f1 >= F1 - reach:
                A[reach + f1 - F1, at] = pltpu.roll(v, 1, 1)
    for f1 in range(F1):
        row = tall + (f1 % 2) * 128 + (f1 // 2) * SUB
        re = wide[row : row + SUB, :LANES]
        im = wide[row : row + SUB, LANES:]
        for k, v in enumerate((re, re + im, re - im)):
            A[f1, REFER + 3 * slot + k] = v


def product(plan, first, f1, index, slots, A, start):
    at = f1 + first + index
    sums = [None] * 3 if start else [A[f1, HELD + 3 * index + k] for k in range(3)]
    for slot in range(slots):
        for k in range(3):
            v = A[at, SIGNAL + 3 * slot + k] * A[f1, REFER + 3 * slot + k]
            sums[k] = v if sums[k] is None else sums[k] + v
    return sums


def add_spectra(plan, first, slots, A, start):
    step = 4

    @pl.loop(0, F1 // step)
    def _(block):
        for k in range(step):
            f1 = block * step + k
            for index in range(plan.mine):
                sums = product(plan, first, f1, index, slots, A, start)
                for which in range(3):
                    A[f1, HELD + 3 * index + which] = sums[which]


def last_spectra(plan, first, slots, owner, A, fold, high, low):
    step = 2

    @pl.loop(0, F1 // step)
    def _(block):
        kept = []
        for k in range(step):
            f1 = block * step + k
            for i in range(plan.per_owner):
                index = owner * plan.per_owner + i
                one, two, three = product(plan, first, f1, index, slots, A, False)
                at = i * (SUB + 1)
                fold[k, 0, at : at + SUB, :] = one - three
                fold[k, 1, at : at + SUB, :] = one - two
            for part in range(2):
                found = [
                    fold[k, part, pl.ds(i, SUB, stride=SUB + 1), :] for i in range(SUB)
                ]
                while len(found) > 1:
                    found = [x + y for x, y in zip(found[::2], found[1::2])]
                kept.append(found[0])
        rows = pl.ds(pl.multiple_of(block * step * SUB, step * SUB), step * SUB)
        for part in range(2):
            h, l = halves(jnp.concatenate(kept[part::2], 0))
            lanes = slice(part * LANES, (part + 1) * LANES)
            high[owner, rows, lanes] = h
            low[owner, rows, lanes] = l


def to_lags(plan, owner, waves, back, high, low, Z, out):
    Z[owner] = lanes_turned(high[owner], low[owner], waves, 2)
    z = []
    for f1 in range(F1):
        rows = slice(f1 * SUB, f1 * SUB + SUB)
        v = (Z[owner, rows, :LANES], Z[owner, rows, LANES:])
        z.append(times_(v, (back[f1, 0], back[f1, 1])))
    half = F1 // 2
    sums = dft16([plus(z[i], z[i + half]) for i in range(half)], 1)
    gaps = dft16([turned(minus(z[i], z[i + half]), i, F1, 1) for i in range(half)], 1)
    for e in range(N1 // 2):
        for parity, found in enumerate((sums, gaps)):
            out[2 * e + parity, owner] = jnp.concatenate(found[e], 0).astype(
                jnp.bfloat16
            )


def gather_and_compute(plan, own, every, ahead, sems, prepared, transform, add):
    send_sems, recv_sems, ahead_send, ahead_recv, own_sems = sems
    cuts, far = plan.cuts, plan.far
    t, c = lax.axis_index("tm"), lax.axis_index("dop")
    z, near = t // 4, t % 4
    beside = [flipped_by(near, k) for k in (1, 2, 3)]
    levels = [z] + [k + (k + far - z) // far for k in range(far - 1)]
    fellows = [flipped_by(c, k) for k in range(1, cuts)]

    sent = []
    pad = (0, ROWS)
    rows = own[0].shape[0]
    me = t * cuts + c

    def place(which, source):
        start = pl.multiple_of(source * rows, rows) + pad[which]
        return every[which].at[pl.ds(pl.multiple_of(start, 16), rows)]

    mine = [
        pltpu.make_async_copy(own[which], place(which, me), own_sems.at[which])
        for which in range(2)
    ]
    for one in mine:
        one.start()

    partners = [(z * 4 + n, c) for n in beside]
    partners += [(other * 4 + near, c) for other in levels[1:]]
    partners += [(t, fellow) for fellow in fellows]
    barrier = pltpu.get_barrier_semaphore()
    for to, cut in partners:
        pl.semaphore_signal(
            barrier, inc=1, device_id={"tm": to, "dop": cut}, device_id_type=MESH
        )
    tail = min(rows, ROWS)
    enders = ROWS // tail
    ends = (near == 3) & (c >= cuts - enders) & (z < far - 1)

    @pl.when(z > 0)
    def _():
        for i in range(enders):
            pl.semaphore_signal(
                barrier,
                inc=1,
                device_id={"tm": t - near - 1, "dop": cuts - enders + i},
                device_id_type=MESH,
            )

    pl.semaphore_wait(barrier, len(partners) + jnp.where(ends, 4 * cuts, 0))

    last = place(1, me).at[pl.ds(rows - tail, tail)]

    def forerun(slot, n, cut):
        which = jnp.maximum(c - (cuts - enders), 0)
        return pltpu.make_async_remote_copy(
            src_ref=last,
            dst_ref=ahead.at[pl.ds(pl.multiple_of(which * tail, tail), tail)],
            send_sem=ahead_send.at[slot],
            recv_sem=ahead_recv.at[which],
            device_id={"tm": jnp.minimum(z + 1, far - 1) * 4 + n, "dop": cut},
            device_id_type=MESH,
        )

    spots = [(n, cut) for n in range(4) for cut in range(cuts)]
    for one in mine:
        one.wait()

    @pl.when(ends)
    def _():
        for slot, (n, cut) in enumerate(spots):
            forerun(slot, n, cut).start()

    def copy(which, source, src, to, cut, slot):
        return pltpu.make_async_remote_copy(
            src_ref=src,
            dst_ref=place(which, source),
            send_sem=send_sems.at[slot],
            recv_sem=recv_sems.at[which, source],
            device_id={"tm": to, "dop": cut},
            device_id_type=MESH,
        )

    def send(source, to, cut):
        for which in range(2):
            one = copy(which, source, place(which, source), to, cut, len(sent))
            one.start()
            sent.append(one)

    def landed(source):
        for which in range(2):
            copy(which, source, place(which, source), t, c, 0).wait_recv()

    def pass_on(k):
        for n in beside:
            source = (levels[k] * 4 + n) * cuts + c
            landed(source)
            for fellow in fellows:
                send(source, t, fellow)

    def complete(k):
        for fellow in fellows:
            for n in [near] + beside:
                landed((levels[k] * 4 + n) * cuts + fellow)

    for level in levels[1:]:
        send(me, level * 4 + near, c)
    for n in beside:
        send(me, z * 4 + n, c)
    for fellow in fellows:
        send(me, t, fellow)
    prepared()

    pass_on(0)
    for level in levels[1:]:
        source = (level * 4 + near) * cuts + c
        landed(source)
        for n in beside:
            send(source, z * 4 + n, c)
        for fellow in fellows:
            send(source, t, fellow)

    @pl.when(z == 0)
    def _():
        ahead[...] = jnp.zeros((ROWS, LANES), jnp.bfloat16)

    @pl.when(z > 0)
    def _():
        for i in range(enders):
            pltpu.make_async_remote_copy(
                src_ref=last,
                dst_ref=ahead.at[pl.ds(i * tail, tail)],
                send_sem=ahead_send.at[0],
                recv_sem=ahead_recv.at[i],
                device_id={"tm": t, "dop": c},
                device_id_type=MESH,
            ).wait_recv()

    for k in range(far):
        complete(k)
        transform([2 * levels[k], 2 * levels[k] + 1], ahead if k == 0 else None)
        if k < far - 1:
            pass_on(k + 1)
        add(k == 0, k == far - 1)

    @pl.when(ends)
    def _():
        for slot, (n, cut) in enumerate(spots):
            forerun(slot, n, cut).wait_send()

    return sent


def sends_needed(plan):
    far, fellows = plan.far, plan.cuts - 1
    return 2 * ((far - 1) + far * (3 + 4 * fellows))


def dealer(plan, tiles, out, sems):
    send_sems, recv_sems = sems
    times = plan.times
    t, c = lax.axis_index("tm"), lax.axis_index("dop")
    me = t * plan.cuts + c
    fine = me // plan.share
    base = (me % plan.share) * plan.owners
    to_me = (base <= c) & (c < base + plan.owners)

    def copy(step, owner):
        to = flipped_by(t, step)
        return pltpu.make_async_remote_copy(
            src_ref=tiles.at[to * plan.lags // LANES, owner],
            dst_ref=out.at[fine],
            send_sem=send_sems.at[step, owner],
            recv_sem=recv_sems.at[fine],
            device_id={"tm": to, "dop": base + owner},
            device_id_type=MESH,
        )

    def start(owner):
        for step in range(times - 1, 0, -1):
            copy(step, owner).start()
        itself = base + owner == c

        @pl.when(jnp.logical_not(itself))
        def _():
            copy(0, owner).start()

        @pl.when(itself)
        def _():
            out[fine] = tiles[t * plan.lags // LANES, owner]

    def finish():
        for source in range(plan.fine):

            @pl.when((fine != source) | jnp.logical_not(to_me))
            def _():
                pltpu.make_async_remote_copy(
                    src_ref=tiles.at[0, 0],
                    dst_ref=out.at[source],
                    send_sem=send_sems.at[0, 0],
                    recv_sem=recv_sems.at[source],
                    device_id={"tm": t, "dop": c},
                    device_id_type=MESH,
                ).wait_recv()

        for step in range(1, times):
            for owner in range(plan.owners):
                copy(step, owner).wait_send()
        for owner in range(plan.owners):

            @pl.when(base + owner != c)
            def _():
                copy(0, owner).wait_send()

    return start, finish


def whole_kernel(plan, s, r, waves_at, forward_at, back_at, out, *scratch):
    (gs, gr, waves, forward, back, tiles) = scratch[:6]
    drift, even, odd, A, ahead, fold = scratch[6:12]
    stage, rstage, high, low, yhigh, ylow, Z = scratch[12:19]
    load_sems, gather_sems, deal_sems = scratch[19], scratch[20:25], scratch[25:27]
    me = lax.axis_index("tm") * plan.cuts + lax.axis_index("dop")
    fine = me // plan.share
    first = 0 if plan.share == 1 else (me % plan.share) * plan.mine
    loads = [
        pltpu.make_async_copy(source, target, load_sems.at[i])
        for i, (source, target) in enumerate(
            ((waves_at, waves), (forward_at, forward), (back_at, back))
        )
    ]

    if plan.per_owner < SUB:
        fold[...] = jnp.zeros(fold.shape, jnp.float32)

    def prepared():
        for load in loads:
            load.start()
        gr[:ROWS, :] = jnp.zeros((ROWS, LANES), jnp.bfloat16)
        prepare(plan, fine, drift, even, odd)
        for load in loads:
            load.wait()

    def transform(groups, before):
        for slot, group in enumerate(groups):
            work = (drift, even, odd, stage, high, low)
            signal_rows(plan, group, slot, gs, forward, work)
            work = (rstage, high, low)
            head = before if slot == 0 else None
            reference_rows(plan, group, slot, gr, head, forward, work)
            group_spectra(plan, slot, waves, high, low, A)

    def add(start, last):
        if last:
            deal = dealer(plan, tiles, out, deal_sems)
            for owner in range(plan.owners):
                last_spectra(plan, first, 2, owner, A, fold, yhigh, ylow)
                to_lags(plan, owner, waves, back, yhigh, ylow, Z, tiles)
                deal[0](owner)
            deal[1]()
        else:
            add_spectra(plan, first, 2, A, start)

    sent = gather_and_compute(
        plan, (s, r), (gs, gr), ahead, gather_sems, prepared, transform, add
    )
    for one in sent:
        one.wait_send()


def dealt_maps(plan, s, r):
    waves, forward, back = tables(plan)
    f32, bf16 = jnp.float32, jnp.bfloat16
    samples = 2 * plan.window // LANES
    slots = 2
    width = -(-(HELD + 3 * plan.mine) // 4) * 4
    enders = max(1, ROWS * plan.devices // samples)
    return pl.pallas_call(
        functools.partial(whole_kernel, plan),
        out_shape=jax.ShapeDtypeStruct((plan.fine, 2 * SUB, LANES), bf16),
        in_specs=[pl.BlockSpec(memory_space=pltpu.MemorySpace.HBM)] * 5,
        out_specs=pl.BlockSpec(memory_space=pltpu.VMEM),
        scratch_shapes=[
            pltpu.VMEM((samples, LANES), bf16),
            pltpu.VMEM((samples + ROWS, LANES), bf16),
            pltpu.VMEM(waves.shape, bf16),
            pltpu.VMEM(forward.shape, f32),
            pltpu.VMEM(back.shape, f32),
            pltpu.VMEM((N1, plan.owners, 2 * SUB, LANES), bf16),
            pltpu.VMEM((plan.groups, 2, SUB, LANES), f32),
            pltpu.VMEM((N1, 2, SUB, LANES), f32),
            pltpu.VMEM((N1, 2, SUB, LANES), f32),
            pltpu.VMEM((F1 + plan.shifts, width, SUB, LANES), f32),
            pltpu.VMEM((ROWS, LANES), bf16),
            pltpu.VMEM((2, 2, SUB * (SUB + 1) + 7, LANES), f32),
            pltpu.VMEM((slots, SUB * APART + 7, LANES), f32),
            pltpu.VMEM((slots, SUB * APART + APART + 7, LANES), f32),
            pltpu.VMEM((slots, 2, F1 * SUB, 2 * LANES), bf16),
            pltpu.VMEM((slots, 2, F1 * SUB, 2 * LANES), bf16),
            pltpu.VMEM((plan.owners, F1 * SUB, 2 * LANES), bf16),
            pltpu.VMEM((plan.owners, F1 * SUB, 2 * LANES), bf16),
            pltpu.VMEM((plan.owners, F1 * SUB, 2 * LANES), f32),
            pltpu.SemaphoreType.DMA((3,)),
            pltpu.SemaphoreType.DMA((sends_needed(plan),)),
            pltpu.SemaphoreType.DMA((2, plan.devices)),
            pltpu.SemaphoreType.DMA((4 * plan.cuts,)),
            pltpu.SemaphoreType.DMA((enders,)),
            pltpu.SemaphoreType.DMA((2,)),
            pltpu.SemaphoreType.DMA((plan.times, plan.owners)),
            pltpu.SemaphoreType.DMA((plan.fine,)),
        ],
        compiler_params=pltpu.CompilerParams(
            collective_id=0,
            has_side_effects=True,
            vmem_limit_bytes=56 * 1024 * 1024,
        ),
    )(s, r, jnp.asarray(waves), jnp.asarray(forward), jnp.asarray(back))


def flipped(index, bit):
    weight = 1 << bit
    return index + weight * (1 - 2 * ((index // weight) % 2))


def flipped_by(index, mask):
    for bit in range(mask.bit_length()):
        if mask >> bit & 1:
            index = flipped(index, bit)
    return index


def order_of(plan):
    bins = F // plan.cuts
    order = np.zeros((plan.fine, 2, SUB, 2, bins), np.float32)
    for fine in range(plan.fine):
        for part in range(2):
            for i in range(plan.per_owner):
                order[fine, part, i, part, plan.fine * i + fine] = 1.0
    return order.reshape(plan.fine * 2 * SUB, 2 * bins).astype(jnp.bfloat16)


def settle_kernel(plan, tiles, order, out):
    rows = plan.fine * 2 * SUB
    wide = lax.dot_general(
        tiles[...].reshape(rows, LANES),
        order[...],
        (((0,), (0,)), ((), ())),
        preferred_element_type=jnp.float32,
    )
    bins = F // plan.cuts
    if plan.lags < LANES:
        pieces = LANES // plan.lags
        which = lax.axis_index("tm") % pieces
        kept = wide[: plan.lags]
        for piece in range(1, pieces):
            kept = jnp.where(
                which == piece, wide[piece * plan.lags : (piece + 1) * plan.lags], kept
            )
        wide = kept
    out[:, 0, :] = wide[:, :bins]
    out[:, 1, :] = wide[:, bins:]


def settled(plan, tiles):
    return pl.pallas_call(
        functools.partial(settle_kernel, plan),
        out_shape=jax.ShapeDtypeStruct((plan.lags, 2, F // plan.cuts), jnp.float32),
        in_specs=[pl.BlockSpec(memory_space=pltpu.VMEM)] * 2,
        out_specs=pl.BlockSpec(memory_space=pltpu.VMEM),
    )(tiles, jnp.asarray(order_of(plan)))


def paired_rows(x):
    samples = x.shape[1] * x.shape[2]
    split = x.reshape(2, samples // LANES, LANES).transpose(1, 0, 2)
    return split.reshape(2 * samples // LANES, LANES)


def on_device(surveillance, reference_signal):
    times, cuts = lax.axis_size("tm"), lax.axis_size("dop")
    samples = surveillance.shape[1] * surveillance.shape[2]
    plan = Plan(times, cuts, samples * times * cuts)
    tiles = dealt_maps(plan, paired_rows(surveillance), paired_rows(reference_signal))
    return settled(plan, tiles)


def solution(mesh):
    return jax.shard_map(
        on_device,
        mesh=mesh,
        in_specs=(P(None, "tm", "dop"), P(None, "tm", "dop")),
        out_specs=P("tm", None, "dop"),
        check_vma=False,
    )
```

```python
import functools
import math

import jax
import jax.numpy as jnp
import numpy as np
from jax import lax
from jax.experimental import pallas as pl
from jax.experimental.pallas import tpu as pltpu
from jax.sharding import PartitionSpec as P

F = 512
LAGS = 2048
LANES = 128
SUB = 8
POINTS = 2 * LAGS
N1 = LAGS // LANES
F1 = POINTS // LANES
ROWS = 2 * N1
GROUP = SUB * ROWS
APART = ROWS + 1
MESH = pl.DeviceIdType.MESH
SIGNAL, REFER, HELD = 0, 6, 12


class Plan:
    def __init__(self, times, cuts, window):
        self.times, self.cuts, self.window = times, cuts, window
        self.devices = times * cuts
        self.groups = window // (SUB * LAGS)
        self.far = times // 4
        self.fine = window // POINTS
        self.shifts = F // self.fine
        self.share = self.devices // self.fine
        self.mine = self.shifts // self.share
        self.per_owner = self.shifts // cuts
        self.owners = self.mine // self.per_owner
        self.lags = LAGS // times


def halves(x):
    high = x.astype(jnp.bfloat16)
    low = (x - high.astype(jnp.float32)).astype(jnp.bfloat16)
    return high, low


def tables(plan):
    a = np.arange(LANES)
    angle = 2.0 * np.pi / LANES * np.mod(a[:, None] * a[None, :], LANES)
    c, s = np.cos(angle), np.sin(angle)
    waves = []
    for sign in (-1.0, 1.0):
        full = np.block([[c, sign * s], [-sign * s, c]])
        high = full.astype(jnp.bfloat16)
        low = (full - high.astype(np.float64)).astype(jnp.bfloat16)
        waves += [high, low]
    turn = 2.0 * np.pi / POINTS * np.arange(F1)[:, None] * a[None, :]
    turns = np.stack([np.cos(turn), -np.sin(turn)], 1)
    sign = np.where(
        (np.arange(F1)[:, None] * np.arange(SUB)[None, :]) % 2 == 1, -1.0, 1.0
    )
    forward = (turns[:, :, None, :] * sign[:, None, :, None]).astype(np.float32)
    scale = 1.0 / (POINTS * math.sqrt(plan.window))
    back = (np.stack([np.cos(turn), np.sin(turn)], 1) * scale).astype(np.float32)
    back = np.broadcast_to(back[:, :, None, :], (F1, 2, SUB, LANES)).copy()
    return np.stack(waves), forward, back


def times_(x, y):
    return x[0] * y[0] - x[1] * y[1], x[0] * y[1] + x[1] * y[0]


def plus(x, y):
    return x[0] + y[0], x[1] + y[1]


def minus(x, y):
    return x[0] - y[0], x[1] - y[1]


def turned(x, numerator, denominator, sign):
    eighth = (8 * numerator) % (8 * denominator) / denominator
    if eighth == 0:
        return x
    if eighth == 4:
        return -x[0], -x[1]
    if eighth in (2, 6):
        if (eighth == 2) == (sign > 0):
            return -x[1], x[0]
        return x[1], -x[0]
    angle = 2.0 * math.pi * numerator / denominator
    c, s = math.cos(angle), sign * math.sin(angle)
    return x[0] * c - x[1] * s, x[1] * c + x[0] * s


def dft4(x, sign):
    a, b = plus(x[0], x[2]), minus(x[0], x[2])
    c, d = plus(x[1], x[3]), turned(minus(x[1], x[3]), 1, 4, sign)
    return [plus(a, c), plus(b, d), minus(a, c), minus(b, d)]


def dft16(x, sign):
    inner = [dft4(x[i::4], sign) for i in range(4)]
    out = [None] * 16
    for k in range(4):
        column = [turned(inner[i][k], i * k, 16, sign) for i in range(4)]
        for j, value in enumerate(dft4(column, sign)):
            out[k + 4 * j] = value
    return out


def phases_of(steps, window):
    angle = lax.bitwise_and(steps, window - 1).astype(jnp.float32) * (
        2.0 * math.pi / window
    )
    return jnp.cos(angle), -jnp.sin(angle)


def prepare(plan, fine, drift, even, odd):
    sub = lax.broadcasted_iota(jnp.int32, (SUB, LANES), 0)
    lane = lax.broadcasted_iota(jnp.int32, (SUB, LANES), 1)

    @pl.loop(0, plan.groups)
    def _(group):
        segment = SUB * group + sub
        c, s = phases_of(fine * (lane + segment * LAGS), plan.window)
        drift[group, 0] = c
        drift[group, 1] = s

    @pl.loop(0, N1)
    def _(row):
        steps = jnp.full((SUB, LANES), fine * LANES * row, jnp.int32)
        c, s = phases_of(steps, plan.window)
        even[row, 0] = c
        even[row, 1] = s
        c, s = phases_of(steps + row * (plan.window // F1), plan.window)
        odd[row, 0] = c
        odd[row, 1] = s


def staged(rows, stage, skip=0):
    for i in range(rows.shape[0] // ROWS):
        at = (i + skip) * APART
        stage[at : at + ROWS, :] = rows[i * ROWS : (i + 1) * ROWS, :].astype(jnp.float32)


def spread_rows(stage, skip=0):
    first = skip * APART
    return [
        tuple(
            stage[pl.ds(first + 2 * n + part, SUB, stride=APART), :]
            for part in range(2)
        )
        for n in range(N1)
    ]


def turn_and_split(found, parity, forward, high, low):
    for pair in range(N1 // 2):
        both = []
        for e in (2 * pair, 2 * pair + 1):
            f1 = 2 * e + parity
            both.append(times_(found[e], (forward[f1, 0], forward[f1, 1])))
        rows = slice(parity * 128 + pair * 16, parity * 128 + pair * 16 + 16)
        for part in range(2):
            h, l = halves(jnp.concatenate([both[0][part], both[1][part]], 0))
            lanes = slice(part * LANES, (part + 1) * LANES)
            high[rows, lanes] = h
            low[rows, lanes] = l


def lanes_turned(high, low, waves, at):
    return (
        jnp.dot(high[...], waves[at], preferred_element_type=jnp.float32)
        + jnp.dot(low[...], waves[at], preferred_element_type=jnp.float32)
        + jnp.dot(high[...], waves[at + 1], preferred_element_type=jnp.float32)
    )


def signal_rows(plan, group, slot, gs, forward, work):
    drift, even, odd, stage, high, low = work
    stage, high, low = stage.at[slot], high.at[slot, 0], low.at[slot, 0]
    start = pl.multiple_of(group * GROUP, GROUP)
    staged(gs[pl.ds(start, GROUP), :], stage)
    here = (drift[group, 0], drift[group, 1])
    x = [times_(v, here) for v in spread_rows(stage)]
    for parity, table in enumerate((even, odd)):
        y = [times_(x[n], (table[n, 0], table[n, 1])) for n in range(N1)]
        turn_and_split(dft16(y, -1), parity, forward, high, low)


def reference_rows(plan, group, slot, gr, before, forward, work):
    stage, high, low = work
    stage, high, low = stage.at[slot], high.at[slot, 1], low.at[slot, 1]
    start = pl.multiple_of(group * GROUP, GROUP)
    if before is None:
        staged(gr[pl.ds(start, GROUP + ROWS), :], stage)
    else:
        staged(before[...], stage)
        own = pl.multiple_of(start + ROWS, ROWS)
        staged(gr[pl.ds(own, GROUP), :], stage, 1)
    before, now = spread_rows(stage), spread_rows(stage, 1)
    y = [plus(a, b) for a, b in zip(now, before)]
    turn_and_split(dft16(y, -1), 0, forward, high, low)
    y = [turned(minus(a, b), n, F1, -1) for n, (a, b) in enumerate(zip(now, before))]
    turn_and_split(dft16(y, -1), 1, forward, high, low)


def group_spectra(plan, slot, waves, high, low, A):
    tall = F1 * SUB
    shape = (2 * tall, 2 * LANES)
    wide = lanes_turned(high[slot].reshape(shape), low[slot].reshape(shape), waves, 0)
    reach = plan.shifts // 2
    for f1 in range(F1):
        row = (f1 % 2) * 128 + (f1 // 2) * SUB
        re = wide[row : row + SUB, :LANES]
        im = wide[row : row + SUB, LANES:]
        for k, v in enumerate((re + im, re, im)):
            at = SIGNAL + 3 * slot + k
            A[reach + f1, at] = v
            if f1 < reach:
                A[reach + f1 + F1, at] = pltpu.roll(v, LANES - 1, 1)
            if f1 >= F1 - reach:
                A[reach + f1 - F1, at] = pltpu.roll(v, 1, 1)
    for f1 in range(F1):
        row = tall + (f1 % 2) * 128 + (f1 // 2) * SUB
        re = wide[row : row + SUB, :LANES]
        im = wide[row : row + SUB, LANES:]
        for k, v in enumerate((re, re + im, re - im)):
            A[f1, REFER + 3 * slot + k] = v


def product(plan, first, f1, index, slots, A, start):
    at = f1 + first + index
    sums = [None] * 3 if start else [A[f1, HELD + 3 * index + k] for k in range(3)]
    for slot in range(slots):
        for k in range(3):
            v = A[at, SIGNAL + 3 * slot + k] * A[f1, REFER + 3 * slot + k]
            sums[k] = v if sums[k] is None else sums[k] + v
    return sums


def add_spectra(plan, first, slots, A, start):
    step = 4

    @pl.loop(0, F1 // step)
    def _(block):
        for k in range(step):
            f1 = block * step + k
            for index in range(plan.mine):
                sums = product(plan, first, f1, index, slots, A, start)
                for which in range(3):
                    A[f1, HELD + 3 * index + which] = sums[which]


def last_spectra(plan, first, slots, owner, A, fold, high, low):
    step = 2

    @pl.loop(0, F1 // step)
    def _(block):
        kept = []
        for k in range(step):
            f1 = block * step + k
            for i in range(plan.per_owner):
                index = owner * plan.per_owner + i
                one, two, three = product(plan, first, f1, index, slots, A, False)
                at = i * (SUB + 1)
                fold[k, 0, at : at + SUB, :] = one - three
                fold[k, 1, at : at + SUB, :] = one - two
            for part in range(2):
                found = [
                    fold[k, part, pl.ds(i, SUB, stride=SUB + 1), :] for i in range(SUB)
                ]
                while len(found) > 1:
                    found = [x + y for x, y in zip(found[::2], found[1::2])]
                kept.append(found[0])
        rows = pl.ds(pl.multiple_of(block * step * SUB, step * SUB), step * SUB)
        for part in range(2):
            h, l = halves(jnp.concatenate(kept[part::2], 0))
            lanes = slice(part * LANES, (part + 1) * LANES)
            high[owner, rows, lanes] = h
            low[owner, rows, lanes] = l


def to_lags(plan, owner, waves, back, high, low, Z, out):
    Z[owner] = lanes_turned(high[owner], low[owner], waves, 2)
    z = []
    for f1 in range(F1):
        rows = slice(f1 * SUB, f1 * SUB + SUB)
        v = (Z[owner, rows, :LANES], Z[owner, rows, LANES:])
        z.append(times_(v, (back[f1, 0], back[f1, 1])))
    half = F1 // 2
    sums = dft16([plus(z[i], z[i + half]) for i in range(half)], 1)
    gaps = dft16([turned(minus(z[i], z[i + half]), i, F1, 1) for i in range(half)], 1)
    for e in range(N1 // 2):
        for parity, found in enumerate((sums, gaps)):
            out[2 * e + parity, owner] = jnp.concatenate(found[e], 0).astype(
                jnp.bfloat16
            )


def gather_and_compute(plan, own, every, ahead, sems, prepared, transform, add):
    send_sems, recv_sems, ahead_send, ahead_recv, own_sems = sems
    cuts, far = plan.cuts, plan.far
    t, c = lax.axis_index("tm"), lax.axis_index("dop")
    z, near = t // 4, t % 4
    beside = [flipped_by(near, k) for k in (1, 2, 3)]
    levels = [z] + [k + (k + far - z) // far for k in range(far - 1)]
    fellows = [flipped_by(c, k) for k in range(1, cuts)]

    sent = []
    pad = (0, ROWS)
    rows = own[0].shape[0]
    me = t * cuts + c

    def place(which, source):
        start = pl.multiple_of(source * rows, rows) + pad[which]
        return every[which].at[pl.ds(pl.multiple_of(start, 16), rows)]

    mine = [
        pltpu.make_async_copy(own[which], place(which, me), own_sems.at[which])
        for which in range(2)
    ]
    for one in mine:
        one.start()

    partners = [(z * 4 + n, c) for n in beside]
    partners += [(other * 4 + near, c) for other in levels[1:]]
    partners += [(t, fellow) for fellow in fellows]
    barrier = pltpu.get_barrier_semaphore()
    for to, cut in partners:
        pl.semaphore_signal(
            barrier, inc=1, device_id={"tm": to, "dop": cut}, device_id_type=MESH
        )
    tail = min(rows, ROWS)
    enders = ROWS // tail
    ends = (near == 3) & (c >= cuts - enders) & (z < far - 1)

    @pl.when(z > 0)
    def _():
        for i in range(enders):
            pl.semaphore_signal(
                barrier,
                inc=1,
                device_id={"tm": t - near - 1, "dop": cuts - enders + i},
                device_id_type=MESH,
            )

    pl.semaphore_wait(barrier, len(partners) + jnp.where(ends, 4 * cuts, 0))

    last = place(1, me).at[pl.ds(rows - tail, tail)]

    def forerun(slot, n, cut):
        which = jnp.maximum(c - (cuts - enders), 0)
        return pltpu.make_async_remote_copy(
            src_ref=last,
            dst_ref=ahead.at[pl.ds(pl.multiple_of(which * tail, tail), tail)],
            send_sem=ahead_send.at[slot],
            recv_sem=ahead_recv.at[which],
            device_id={"tm": jnp.minimum(z + 1, far - 1) * 4 + n, "dop": cut},
            device_id_type=MESH,
        )

    spots = [(n, cut) for n in range(4) for cut in range(cuts)]
    for one in mine:
        one.wait()

    @pl.when(ends)
    def _():
        for slot, (n, cut) in enumerate(spots):
            forerun(slot, n, cut).start()

    def copy(which, source, src, to, cut, slot):
        return pltpu.make_async_remote_copy(
            src_ref=src,
            dst_ref=place(which, source),
            send_sem=send_sems.at[slot],
            recv_sem=recv_sems.at[which, source],
            device_id={"tm": to, "dop": cut},
            device_id_type=MESH,
        )

    def send(source, to, cut):
        for which in range(2):
            one = copy(which, source, place(which, source), to, cut, len(sent))
            one.start()
            sent.append(one)

    def landed(source):
        for which in range(2):
            copy(which, source, place(which, source), t, c, 0).wait_recv()

    def pass_on(k):
        for n in beside:
            source = (levels[k] * 4 + n) * cuts + c
            landed(source)
            for fellow in fellows:
                send(source, t, fellow)

    def complete(k):
        for fellow in fellows:
            for n in [near] + beside:
                landed((levels[k] * 4 + n) * cuts + fellow)

    for i in range(1, far):
        level = jnp.where(z < far // 2, levels[far - i], levels[i])
        send(me, level * 4 + near, c)
    for n in beside[::-1]:
        send(me, z * 4 + n, c)
    for fellow in fellows:
        send(me, t, fellow)
    prepared()

    for k, level in enumerate(levels[1:]):
        if k == 1:
            pass_on(0)
        source = (level * 4 + near) * cuts + c
        landed(source)
        for n in beside[::-1]:
            send(source, z * 4 + n, c)
        for fellow in fellows:
            send(source, t, fellow)

    @pl.when(z == 0)
    def _():
        ahead[...] = jnp.zeros((ROWS, LANES), jnp.bfloat16)

    @pl.when(z > 0)
    def _():
        for i in range(enders):
            pltpu.make_async_remote_copy(
                src_ref=last,
                dst_ref=ahead.at[pl.ds(i * tail, tail)],
                send_sem=ahead_send.at[0],
                recv_sem=ahead_recv.at[i],
                device_id={"tm": t, "dop": c},
                device_id_type=MESH,
            ).wait_recv()

    for k in range(far):
        complete(k)
        transform([2 * levels[k], 2 * levels[k] + 1], ahead if k == 0 else None)
        if k < far - 1:
            pass_on(k + 1)
        add(k == 0, k == far - 1)

    @pl.when(ends)
    def _():
        for slot, (n, cut) in enumerate(spots):
            forerun(slot, n, cut).wait_send()

    return sent


def sends_needed(plan):
    far, fellows = plan.far, plan.cuts - 1
    return 2 * ((far - 1) + far * (3 + 4 * fellows))


def dealer(plan, tiles, out, sems):
    send_sems, recv_sems = sems
    times = plan.times
    t, c = lax.axis_index("tm"), lax.axis_index("dop")
    me = t * plan.cuts + c
    fine = me // plan.share
    base = (me % plan.share) * plan.owners
    to_me = (base <= c) & (c < base + plan.owners)

    def copy(step, owner):
        to = flipped_by(t, step)
        return pltpu.make_async_remote_copy(
            src_ref=tiles.at[to * plan.lags // LANES, owner],
            dst_ref=out.at[fine],
            send_sem=send_sems.at[step, owner],
            recv_sem=recv_sems.at[fine],
            device_id={"tm": to, "dop": base + owner},
            device_id_type=MESH,
        )

    def start(owner):
        for step in range(times - 1, 0, -1):
            copy(step, owner).start()
        itself = base + owner == c

        @pl.when(jnp.logical_not(itself))
        def _():
            copy(0, owner).start()

        @pl.when(itself)
        def _():
            out[fine] = tiles[t * plan.lags // LANES, owner]

    def finish():
        for source in range(plan.fine):

            @pl.when((fine != source) | jnp.logical_not(to_me))
            def _():
                pltpu.make_async_remote_copy(
                    src_ref=tiles.at[0, 0],
                    dst_ref=out.at[source],
                    send_sem=send_sems.at[0, 0],
                    recv_sem=recv_sems.at[source],
                    device_id={"tm": t, "dop": c},
                    device_id_type=MESH,
                ).wait_recv()

        for step in range(1, times):
            for owner in range(plan.owners):
                copy(step, owner).wait_send()
        for owner in range(plan.owners):

            @pl.when(base + owner != c)
            def _():
                copy(0, owner).wait_send()

    return start, finish


def whole_kernel(plan, s, r, waves_at, forward_at, back_at, out, *scratch):
    (gs, gr, waves, forward, back, tiles) = scratch[:6]
    drift, even, odd, A, ahead, fold = scratch[6:12]
    stage, rstage, high, low, yhigh, ylow, Z = scratch[12:19]
    load_sems, gather_sems, deal_sems = scratch[19], scratch[20:25], scratch[25:27]
    me = lax.axis_index("tm") * plan.cuts + lax.axis_index("dop")
    fine = me // plan.share
    first = 0 if plan.share == 1 else (me % plan.share) * plan.mine
    loads = [
        pltpu.make_async_copy(source, target, load_sems.at[i])
        for i, (source, target) in enumerate(
            ((waves_at, waves), (forward_at, forward), (back_at, back))
        )
    ]

    if plan.per_owner < SUB:
        fold[...] = jnp.zeros(fold.shape, jnp.float32)

    def prepared():
        for load in loads:
            load.start()
        gr[:ROWS, :] = jnp.zeros((ROWS, LANES), jnp.bfloat16)
        prepare(plan, fine, drift, even, odd)
        for load in loads:
            load.wait()

    def transform(groups, before):
        for slot, group in enumerate(groups):
            work = (drift, even, odd, stage, high, low)
            signal_rows(plan, group, slot, gs, forward, work)
            work = (rstage, high, low)
            head = before if slot == 0 else None
            reference_rows(plan, group, slot, gr, head, forward, work)
            group_spectra(plan, slot, waves, high, low, A)

    def add(start, last):
        if last:
            deal = dealer(plan, tiles, out, deal_sems)
            for owner in range(plan.owners):
                last_spectra(plan, first, 2, owner, A, fold, yhigh, ylow)
                to_lags(plan, owner, waves, back, yhigh, ylow, Z, tiles)
                deal[0](owner)
            deal[1]()
        else:
            add_spectra(plan, first, 2, A, start)

    sent = gather_and_compute(
        plan, (s, r), (gs, gr), ahead, gather_sems, prepared, transform, add
    )
    for one in sent:
        one.wait_send()


def dealt_maps(plan, s, r):
    waves, forward, back = tables(plan)
    f32, bf16 = jnp.float32, jnp.bfloat16
    samples = 2 * plan.window // LANES
    slots = 2
    width = -(-(HELD + 3 * plan.mine) // 4) * 4
    enders = max(1, ROWS * plan.devices // samples)
    return pl.pallas_call(
        functools.partial(whole_kernel, plan),
        out_shape=jax.ShapeDtypeStruct((plan.fine, 2 * SUB, LANES), bf16),
        in_specs=[pl.BlockSpec(memory_space=pltpu.MemorySpace.HBM)] * 5,
        out_specs=pl.BlockSpec(memory_space=pltpu.VMEM),
        scratch_shapes=[
            pltpu.VMEM((samples, LANES), bf16),
            pltpu.VMEM((samples + ROWS, LANES), bf16),
            pltpu.VMEM(waves.shape, bf16),
            pltpu.VMEM(forward.shape, f32),
            pltpu.VMEM(back.shape, f32),
            pltpu.VMEM((N1, plan.owners, 2 * SUB, LANES), bf16),
            pltpu.VMEM((plan.groups, 2, SUB, LANES), f32),
            pltpu.VMEM((N1, 2, SUB, LANES), f32),
            pltpu.VMEM((N1, 2, SUB, LANES), f32),
            pltpu.VMEM((F1 + plan.shifts, width, SUB, LANES), f32),
            pltpu.VMEM((ROWS, LANES), bf16),
            pltpu.VMEM((2, 2, SUB * (SUB + 1) + 7, LANES), f32),
            pltpu.VMEM((slots, SUB * APART + 7, LANES), f32),
            pltpu.VMEM((slots, SUB * APART + APART + 7, LANES), f32),
            pltpu.VMEM((slots, 2, F1 * SUB, 2 * LANES), bf16),
            pltpu.VMEM((slots, 2, F1 * SUB, 2 * LANES), bf16),
            pltpu.VMEM((plan.owners, F1 * SUB, 2 * LANES), bf16),
            pltpu.VMEM((plan.owners, F1 * SUB, 2 * LANES), bf16),
            pltpu.VMEM((plan.owners, F1 * SUB, 2 * LANES), f32),
            pltpu.SemaphoreType.DMA((3,)),
            pltpu.SemaphoreType.DMA((sends_needed(plan),)),
            pltpu.SemaphoreType.DMA((2, plan.devices)),
            pltpu.SemaphoreType.DMA((4 * plan.cuts,)),
            pltpu.SemaphoreType.DMA((enders,)),
            pltpu.SemaphoreType.DMA((2,)),
            pltpu.SemaphoreType.DMA((plan.times, plan.owners)),
            pltpu.SemaphoreType.DMA((plan.fine,)),
        ],
        compiler_params=pltpu.CompilerParams(
            collective_id=0,
            has_side_effects=True,
            vmem_limit_bytes=56 * 1024 * 1024,
        ),
    )(s, r, jnp.asarray(waves), jnp.asarray(forward), jnp.asarray(back))


def flipped(index, bit):
    weight = 1 << bit
    return index + weight * (1 - 2 * ((index // weight) % 2))


def flipped_by(index, mask):
    for bit in range(mask.bit_length()):
        if mask >> bit & 1:
            index = flipped(index, bit)
    return index


def order_of(plan):
    bins = F // plan.cuts
    order = np.zeros((plan.fine, 2, SUB, 2, bins), np.float32)
    for fine in range(plan.fine):
        for part in range(2):
            for i in range(plan.per_owner):
                order[fine, part, i, part, plan.fine * i + fine] = 1.0
    return order.reshape(plan.fine * 2 * SUB, 2 * bins).astype(jnp.bfloat16)


def settle_kernel(plan, tiles, order, out):
    rows = plan.fine * 2 * SUB
    wide = lax.dot_general(
        tiles[...].reshape(rows, LANES),
        order[...],
        (((0,), (0,)), ((), ())),
        preferred_element_type=jnp.float32,
    )
    bins = F // plan.cuts
    if plan.lags < LANES:
        pieces = LANES // plan.lags
        which = lax.axis_index("tm") % pieces
        kept = wide[: plan.lags]
        for piece in range(1, pieces):
            kept = jnp.where(
                which == piece, wide[piece * plan.lags : (piece + 1) * plan.lags], kept
            )
        wide = kept
    out[:, 0, :] = wide[:, :bins]
    out[:, 1, :] = wide[:, bins:]


def settled(plan, tiles):
    return pl.pallas_call(
        functools.partial(settle_kernel, plan),
        out_shape=jax.ShapeDtypeStruct((plan.lags, 2, F // plan.cuts), jnp.float32),
        in_specs=[pl.BlockSpec(memory_space=pltpu.VMEM)] * 2,
        out_specs=pl.BlockSpec(memory_space=pltpu.VMEM),
    )(tiles, jnp.asarray(order_of(plan)))


def paired_rows(x):
    samples = x.shape[1] * x.shape[2]
    split = x.reshape(2, samples // LANES, LANES).transpose(1, 0, 2)
    return split.reshape(2 * samples // LANES, LANES)


def on_device(surveillance, reference_signal):
    times, cuts = lax.axis_size("tm"), lax.axis_size("dop")
    samples = surveillance.shape[1] * surveillance.shape[2]
    plan = Plan(times, cuts, samples * times * cuts)
    tiles = dealt_maps(plan, paired_rows(surveillance), paired_rows(reference_signal))
    return settled(plan, tiles)


def solution(mesh):
    return jax.shard_map(
        on_device,
        mesh=mesh,
        in_specs=(P(None, "tm", "dop"), P(None, "tm", "dop")),
        out_specs=P("tm", None, "dop"),
        check_vma=False,
    )
```

```python
import functools
import math

import jax
import jax.numpy as jnp
import numpy as np
from jax import lax
from jax.experimental import pallas as pl
from jax.experimental.pallas import tpu as pltpu
from jax.sharding import PartitionSpec as P

F = 512
LAGS = 2048
LANES = 128
SUB = 8
POINTS = 2 * LAGS
N1 = LAGS // LANES
F1 = POINTS // LANES
ROWS = 2 * N1
GROUP = SUB * ROWS
APART = ROWS + 1
MESH = pl.DeviceIdType.MESH
SIGNAL, REFER, HELD = 0, 6, 12


class Plan:
    def __init__(self, times, cuts, window):
        self.times, self.cuts, self.window = times, cuts, window
        self.devices = times * cuts
        self.groups = window // (SUB * LAGS)
        self.far = times // 4
        self.fine = window // POINTS
        self.shifts = F // self.fine
        self.share = self.devices // self.fine
        self.mine = self.shifts // self.share
        self.per_owner = self.shifts // cuts
        self.owners = self.mine // self.per_owner
        self.lags = LAGS // times


def halves(x):
    high = x.astype(jnp.bfloat16)
    low = (x - high.astype(jnp.float32)).astype(jnp.bfloat16)
    return high, low


def tables(plan):
    a = np.arange(LANES)
    angle = 2.0 * np.pi / LANES * np.mod(a[:, None] * a[None, :], LANES)
    c, s = np.cos(angle), np.sin(angle)
    waves = []
    for sign in (-1.0, 1.0):
        full = np.block([[c, sign * s], [-sign * s, c]])
        high = full.astype(jnp.bfloat16)
        low = (full - high.astype(np.float64)).astype(jnp.bfloat16)
        waves += [high, low]
    turn = 2.0 * np.pi / POINTS * np.arange(F1)[:, None] * a[None, :]
    turns = np.stack([np.cos(turn), -np.sin(turn)], 1)
    sign = np.where(
        (np.arange(F1)[:, None] * np.arange(SUB)[None, :]) % 2 == 1, -1.0, 1.0
    )
    forward = (turns[:, :, None, :] * sign[:, None, :, None]).astype(np.float32)
    scale = 1.0 / (POINTS * math.sqrt(plan.window))
    back = (np.stack([np.cos(turn), np.sin(turn)], 1) * scale).astype(np.float32)
    back = np.broadcast_to(back[:, :, None, :], (F1, 2, SUB, LANES)).copy()
    return np.stack(waves), forward, back


def times_(x, y):
    return x[0] * y[0] - x[1] * y[1], x[0] * y[1] + x[1] * y[0]


def plus(x, y):
    return x[0] + y[0], x[1] + y[1]


def minus(x, y):
    return x[0] - y[0], x[1] - y[1]


def turned(x, numerator, denominator, sign):
    eighth = (8 * numerator) % (8 * denominator) / denominator
    if eighth == 0:
        return x
    if eighth == 4:
        return -x[0], -x[1]
    if eighth in (2, 6):
        if (eighth == 2) == (sign > 0):
            return -x[1], x[0]
        return x[1], -x[0]
    angle = 2.0 * math.pi * numerator / denominator
    c, s = math.cos(angle), sign * math.sin(angle)
    return x[0] * c - x[1] * s, x[1] * c + x[0] * s


def dft4(x, sign):
    a, b = plus(x[0], x[2]), minus(x[0], x[2])
    c, d = plus(x[1], x[3]), turned(minus(x[1], x[3]), 1, 4, sign)
    return [plus(a, c), plus(b, d), minus(a, c), minus(b, d)]


def dft16(x, sign):
    inner = [dft4(x[i::4], sign) for i in range(4)]
    out = [None] * 16
    for k in range(4):
        column = [turned(inner[i][k], i * k, 16, sign) for i in range(4)]
        for j, value in enumerate(dft4(column, sign)):
            out[k + 4 * j] = value
    return out


def phases_of(steps, window):
    angle = lax.bitwise_and(steps, window - 1).astype(jnp.float32) * (
        2.0 * math.pi / window
    )
    return jnp.cos(angle), -jnp.sin(angle)


def prepare(plan, fine, drift, even, odd):
    sub = lax.broadcasted_iota(jnp.int32, (SUB, LANES), 0)
    lane = lax.broadcasted_iota(jnp.int32, (SUB, LANES), 1)

    @pl.loop(0, plan.groups)
    def _(group):
        segment = SUB * group + sub
        c, s = phases_of(fine * (lane + segment * LAGS), plan.window)
        drift[group, 0] = c
        drift[group, 1] = s

    @pl.loop(0, N1)
    def _(row):
        steps = jnp.full((SUB, LANES), fine * LANES * row, jnp.int32)
        c, s = phases_of(steps, plan.window)
        even[row, 0] = c
        even[row, 1] = s
        c, s = phases_of(steps + row * (plan.window // F1), plan.window)
        odd[row, 0] = c
        odd[row, 1] = s


def staged(rows, stage, skip=0):
    for i in range(rows.shape[0] // ROWS):
        at = (i + skip) * APART
        stage[at : at + ROWS, :] = rows[i * ROWS : (i + 1) * ROWS, :].astype(jnp.float32)


def spread_rows(stage, skip=0):
    first = skip * APART
    return [
        tuple(
            stage[pl.ds(first + 2 * n + part, SUB, stride=APART), :]
            for part in range(2)
        )
        for n in range(N1)
    ]


def turn_and_split(found, parity, forward, high, low):
    for pair in range(N1 // 2):
        both = []
        for e in (2 * pair, 2 * pair + 1):
            f1 = 2 * e + parity
            both.append(times_(found[e], (forward[f1, 0], forward[f1, 1])))
        rows = slice(parity * 128 + pair * 16, parity * 128 + pair * 16 + 16)
        for part in range(2):
            h, l = halves(jnp.concatenate([both[0][part], both[1][part]], 0))
            lanes = slice(part * LANES, (part + 1) * LANES)
            high[rows, lanes] = h
            low[rows, lanes] = l


def lanes_turned(high, low, waves, at):
    return (
        jnp.dot(high[...], waves[at], preferred_element_type=jnp.float32)
        + jnp.dot(low[...], waves[at], preferred_element_type=jnp.float32)
        + jnp.dot(high[...], waves[at + 1], preferred_element_type=jnp.float32)
    )


def signal_rows(plan, group, slot, gs, forward, work):
    drift, even, odd, stage, high, low = work
    stage, high, low = stage.at[slot], high.at[slot, 0], low.at[slot, 0]
    start = pl.multiple_of(group * GROUP, GROUP)
    staged(gs[pl.ds(start, GROUP), :], stage)
    here = (drift[group, 0], drift[group, 1])
    x = [times_(v, here) for v in spread_rows(stage)]
    for parity, table in enumerate((even, odd)):
        y = [times_(x[n], (table[n, 0], table[n, 1])) for n in range(N1)]
        turn_and_split(dft16(y, -1), parity, forward, high, low)


def reference_rows(plan, group, slot, gr, before, forward, work):
    stage, high, low = work
    stage, high, low = stage.at[slot], high.at[slot, 1], low.at[slot, 1]
    start = pl.multiple_of(group * GROUP, GROUP)
    if before is None:
        staged(gr[pl.ds(start, GROUP + ROWS), :], stage)
    else:
        staged(before[...], stage)
        own = pl.multiple_of(start + ROWS, ROWS)
        staged(gr[pl.ds(own, GROUP), :], stage, 1)
    before, now = spread_rows(stage), spread_rows(stage, 1)
    y = [plus(a, b) for a, b in zip(now, before)]
    turn_and_split(dft16(y, -1), 0, forward, high, low)
    y = [turned(minus(a, b), n, F1, -1) for n, (a, b) in enumerate(zip(now, before))]
    turn_and_split(dft16(y, -1), 1, forward, high, low)


def group_spectra(plan, slot, waves, high, low, A):
    tall = F1 * SUB
    shape = (2 * tall, 2 * LANES)
    wide = lanes_turned(high[slot].reshape(shape), low[slot].reshape(shape), waves, 0)
    reach = plan.shifts // 2
    for f1 in range(F1):
        row = (f1 % 2) * 128 + (f1 // 2) * SUB
        re = wide[row : row + SUB, :LANES]
        im = wide[row : row + SUB, LANES:]
        for k, v in enumerate((re + im, re, im)):
            at = SIGNAL + 3 * slot + k
            A[reach + f1, at] = v
            if f1 < reach:
                A[reach + f1 + F1, at] = pltpu.roll(v, LANES - 1, 1)
            if f1 >= F1 - reach:
                A[reach + f1 - F1, at] = pltpu.roll(v, 1, 1)
    for f1 in range(F1):
        row = tall + (f1 % 2) * 128 + (f1 // 2) * SUB
        re = wide[row : row + SUB, :LANES]
        im = wide[row : row + SUB, LANES:]
        for k, v in enumerate((re, re + im, re - im)):
            A[f1, REFER + 3 * slot + k] = v


def product(plan, first, f1, index, slots, A, start):
    at = f1 + first + index
    sums = [None] * 3 if start else [A[f1, HELD + 3 * index + k] for k in range(3)]
    for slot in range(slots):
        for k in range(3):
            v = A[at, SIGNAL + 3 * slot + k] * A[f1, REFER + 3 * slot + k]
            sums[k] = v if sums[k] is None else sums[k] + v
    return sums


def add_spectra(plan, first, slots, A, start):
    step = 4

    @pl.loop(0, F1 // step)
    def _(block):
        for k in range(step):
            f1 = block * step + k
            for index in range(plan.mine):
                sums = product(plan, first, f1, index, slots, A, start)
                for which in range(3):
                    A[f1, HELD + 3 * index + which] = sums[which]


def last_spectra(plan, first, slots, owner, A, fold, high, low):
    step = 2

    @pl.loop(0, F1 // step)
    def _(block):
        kept = []
        for k in range(step):
            f1 = block * step + k
            for i in range(plan.per_owner):
                index = owner * plan.per_owner + i
                one, two, three = product(plan, first, f1, index, slots, A, False)
                at = i * (SUB + 1)
                fold[k, 0, at : at + SUB, :] = one - three
                fold[k, 1, at : at + SUB, :] = one - two
            for part in range(2):
                found = [
                    fold[k, part, pl.ds(i, SUB, stride=SUB + 1), :] for i in range(SUB)
                ]
                while len(found) > 1:
                    found = [x + y for x, y in zip(found[::2], found[1::2])]
                kept.append(found[0])
        rows = pl.ds(pl.multiple_of(block * step * SUB, step * SUB), step * SUB)
        for part in range(2):
            h, l = halves(jnp.concatenate(kept[part::2], 0))
            lanes = slice(part * LANES, (part + 1) * LANES)
            high[owner, rows, lanes] = h
            low[owner, rows, lanes] = l


def to_lags(plan, owner, waves, back, high, low, Z, out):
    Z[owner] = lanes_turned(high[owner], low[owner], waves, 2)
    z = []
    for f1 in range(F1):
        rows = slice(f1 * SUB, f1 * SUB + SUB)
        v = (Z[owner, rows, :LANES], Z[owner, rows, LANES:])
        z.append(times_(v, (back[f1, 0], back[f1, 1])))
    half = F1 // 2
    sums = dft16([plus(z[i], z[i + half]) for i in range(half)], 1)
    gaps = dft16([turned(minus(z[i], z[i + half]), i, F1, 1) for i in range(half)], 1)
    for e in range(N1 // 2):
        for parity, found in enumerate((sums, gaps)):
            out[2 * e + parity, owner] = jnp.concatenate(found[e], 0).astype(
                jnp.bfloat16
            )


def gather_and_compute(plan, own, every, ahead, sems, prepared, transform, add):
    send_sems, recv_sems, ahead_send, ahead_recv, own_sems = sems
    cuts, far = plan.cuts, plan.far
    t, c = lax.axis_index("tm"), lax.axis_index("dop")
    z, near = t // 4, t % 4
    beside = [flipped_by(near, k) for k in (1, 2, 3)]
    levels = [z] + [k + (k + far - z) // far for k in range(far - 1)]
    fellows = [flipped_by(c, k) for k in range(1, cuts)]

    sent = []
    pad = (0, ROWS)
    rows = own[0].shape[0]
    me = t * cuts + c

    def place(which, source):
        start = pl.multiple_of(source * rows, rows) + pad[which]
        return every[which].at[pl.ds(pl.multiple_of(start, 16), rows)]

    mine = [
        pltpu.make_async_copy(own[which], place(which, me), own_sems.at[which])
        for which in range(2)
    ]
    for one in mine:
        one.start()

    partners = [(z * 4 + n, c) for n in beside]
    partners += [(other * 4 + near, c) for other in levels[1:]]
    partners += [(t, fellow) for fellow in fellows]
    barrier = pltpu.get_barrier_semaphore()
    for to, cut in partners:
        pl.semaphore_signal(
            barrier, inc=1, device_id={"tm": to, "dop": cut}, device_id_type=MESH
        )
    tail = min(rows, ROWS)
    enders = ROWS // tail
    ends = (near == 3) & (c >= cuts - enders) & (z < far - 1)

    @pl.when(z > 0)
    def _():
        for i in range(enders):
            pl.semaphore_signal(
                barrier,
                inc=1,
                device_id={"tm": t - near - 1, "dop": cuts - enders + i},
                device_id_type=MESH,
            )

    pl.semaphore_wait(barrier, len(partners) + jnp.where(ends, 4 * cuts, 0))

    last = place(1, me).at[pl.ds(rows - tail, tail)]

    def forerun(slot, n, cut):
        which = jnp.maximum(c - (cuts - enders), 0)
        return pltpu.make_async_remote_copy(
            src_ref=last,
            dst_ref=ahead.at[pl.ds(pl.multiple_of(which * tail, tail), tail)],
            send_sem=ahead_send.at[slot],
            recv_sem=ahead_recv.at[which],
            device_id={"tm": jnp.minimum(z + 1, far - 1) * 4 + n, "dop": cut},
            device_id_type=MESH,
        )

    spots = [(n, cut) for n in range(4) for cut in range(cuts)]
    for one in mine:
        one.wait()

    def copy(which, source, src, to, cut, slot):
        return pltpu.make_async_remote_copy(
            src_ref=src,
            dst_ref=place(which, source),
            send_sem=send_sems.at[slot],
            recv_sem=recv_sems.at[which, source],
            device_id={"tm": to, "dop": cut},
            device_id_type=MESH,
        )

    def send(source, to, cut):
        for which in range(2):
            one = copy(which, source, place(which, source), to, cut, len(sent))
            one.start()
            sent.append(one)

    def landed(source):
        for which in range(2):
            copy(which, source, place(which, source), t, c, 0).wait_recv()

    def pass_on(k):
        for n in beside:
            source = (levels[k] * 4 + n) * cuts + c
            landed(source)
            for fellow in fellows:
                send(source, t, fellow)

    def complete(k):
        for fellow in fellows:
            for n in [near] + beside:
                landed((levels[k] * 4 + n) * cuts + fellow)

    for i in range(1, far):
        level = jnp.where(z < far // 2, levels[far - i], levels[i])
        send(me, level * 4 + near, c)
    for n in beside[::-1]:
        send(me, z * 4 + n, c)
    for fellow in fellows:
        send(me, t, fellow)
    @pl.when(ends)
    def _():
        for slot, (n, cut) in enumerate(spots):
            forerun(slot, n, cut).start()

    prepared()

    for k, level in enumerate(levels[1:]):
        if k == 1:
            pass_on(0)
        source = (level * 4 + near) * cuts + c
        landed(source)
        for n in beside[::-1]:
            send(source, z * 4 + n, c)
        for fellow in fellows:
            send(source, t, fellow)

    @pl.when(z == 0)
    def _():
        ahead[...] = jnp.zeros((ROWS, LANES), jnp.bfloat16)

    @pl.when(z > 0)
    def _():
        for i in range(enders):
            pltpu.make_async_remote_copy(
                src_ref=last,
                dst_ref=ahead.at[pl.ds(i * tail, tail)],
                send_sem=ahead_send.at[0],
                recv_sem=ahead_recv.at[i],
                device_id={"tm": t, "dop": c},
                device_id_type=MESH,
            ).wait_recv()

    for k in range(far):
        complete(k)
        transform([2 * levels[k], 2 * levels[k] + 1], ahead if k == 0 else None)
        if k < far - 1:
            pass_on(k + 1)
        add(k == 0, k == far - 1)

    @pl.when(ends)
    def _():
        for slot, (n, cut) in enumerate(spots):
            forerun(slot, n, cut).wait_send()

    return sent


def sends_needed(plan):
    far, fellows = plan.far, plan.cuts - 1
    return 2 * ((far - 1) + far * (3 + 4 * fellows))


def dealer(plan, tiles, out, sems):
    send_sems, recv_sems = sems
    times = plan.times
    t, c = lax.axis_index("tm"), lax.axis_index("dop")
    me = t * plan.cuts + c
    fine = me // plan.share
    base = (me % plan.share) * plan.owners
    to_me = (base <= c) & (c < base + plan.owners)

    def copy(step, owner):
        to = flipped_by(t, step)
        return pltpu.make_async_remote_copy(
            src_ref=tiles.at[to * plan.lags // LANES, owner],
            dst_ref=out.at[fine],
            send_sem=send_sems.at[step, owner],
            recv_sem=recv_sems.at[fine],
            device_id={"tm": to, "dop": base + owner},
            device_id_type=MESH,
        )

    def start(owner):
        for step in range(times - 1, 0, -1):
            copy(step, owner).start()
        itself = base + owner == c

        @pl.when(jnp.logical_not(itself))
        def _():
            copy(0, owner).start()

        @pl.when(itself)
        def _():
            out[fine] = tiles[t * plan.lags // LANES, owner]

    def finish():
        for source in range(plan.fine):

            @pl.when((fine != source) | jnp.logical_not(to_me))
            def _():
                pltpu.make_async_remote_copy(
                    src_ref=tiles.at[0, 0],
                    dst_ref=out.at[source],
                    send_sem=send_sems.at[0, 0],
                    recv_sem=recv_sems.at[source],
                    device_id={"tm": t, "dop": c},
                    device_id_type=MESH,
                ).wait_recv()

        for step in range(1, times):
            for owner in range(plan.owners):
                copy(step, owner).wait_send()
        for owner in range(plan.owners):

            @pl.when(base + owner != c)
            def _():
                copy(0, owner).wait_send()

    return start, finish


def whole_kernel(plan, s, r, waves_at, forward_at, back_at, out, *scratch):
    (gs, gr, waves, forward, back, tiles) = scratch[:6]
    drift, even, odd, A, ahead, fold = scratch[6:12]
    stage, rstage, high, low, yhigh, ylow, Z = scratch[12:19]
    load_sems, gather_sems, deal_sems = scratch[19], scratch[20:25], scratch[25:27]
    me = lax.axis_index("tm") * plan.cuts + lax.axis_index("dop")
    fine = me // plan.share
    first = 0 if plan.share == 1 else (me % plan.share) * plan.mine
    loads = [
        pltpu.make_async_copy(source, target, load_sems.at[i])
        for i, (source, target) in enumerate(
            ((waves_at, waves), (forward_at, forward), (back_at, back))
        )
    ]

    if plan.per_owner < SUB:
        fold[...] = jnp.zeros(fold.shape, jnp.float32)

    def prepared():
        for load in loads:
            load.start()
        gr[:ROWS, :] = jnp.zeros((ROWS, LANES), jnp.bfloat16)
        prepare(plan, fine, drift, even, odd)
        for load in loads:
            load.wait()

    def transform(groups, before):
        for slot, group in enumerate(groups):
            work = (drift, even, odd, stage, high, low)
            signal_rows(plan, group, slot, gs, forward, work)
            work = (rstage, high, low)
            head = before if slot == 0 else None
            reference_rows(plan, group, slot, gr, head, forward, work)
            group_spectra(plan, slot, waves, high, low, A)

    def add(start, last):
        if last:
            deal = dealer(plan, tiles, out, deal_sems)
            for owner in range(plan.owners):
                last_spectra(plan, first, 2, owner, A, fold, yhigh, ylow)
                to_lags(plan, owner, waves, back, yhigh, ylow, Z, tiles)
                deal[0](owner)
            deal[1]()
        else:
            add_spectra(plan, first, 2, A, start)

    sent = gather_and_compute(
        plan, (s, r), (gs, gr), ahead, gather_sems, prepared, transform, add
    )
    for one in sent:
        one.wait_send()


def dealt_maps(plan, s, r):
    waves, forward, back = tables(plan)
    f32, bf16 = jnp.float32, jnp.bfloat16
    samples = 2 * plan.window // LANES
    slots = 2
    width = -(-(HELD + 3 * plan.mine) // 4) * 4
    enders = max(1, ROWS * plan.devices // samples)
    return pl.pallas_call(
        functools.partial(whole_kernel, plan),
        out_shape=jax.ShapeDtypeStruct((plan.fine, 2 * SUB, LANES), bf16),
        in_specs=[pl.BlockSpec(memory_space=pltpu.MemorySpace.HBM)] * 5,
        out_specs=pl.BlockSpec(memory_space=pltpu.VMEM),
        scratch_shapes=[
            pltpu.VMEM((samples, LANES), bf16),
            pltpu.VMEM((samples + ROWS, LANES), bf16),
            pltpu.VMEM(waves.shape, bf16),
            pltpu.VMEM(forward.shape, f32),
            pltpu.VMEM(back.shape, f32),
            pltpu.VMEM((N1, plan.owners, 2 * SUB, LANES), bf16),
            pltpu.VMEM((plan.groups, 2, SUB, LANES), f32),
            pltpu.VMEM((N1, 2, SUB, LANES), f32),
            pltpu.VMEM((N1, 2, SUB, LANES), f32),
            pltpu.VMEM((F1 + plan.shifts, width, SUB, LANES), f32),
            pltpu.VMEM((ROWS, LANES), bf16),
            pltpu.VMEM((2, 2, SUB * (SUB + 1) + 7, LANES), f32),
            pltpu.VMEM((slots, SUB * APART + 7, LANES), f32),
            pltpu.VMEM((slots, SUB * APART + APART + 7, LANES), f32),
            pltpu.VMEM((slots, 2, F1 * SUB, 2 * LANES), bf16),
            pltpu.VMEM((slots, 2, F1 * SUB, 2 * LANES), bf16),
            pltpu.VMEM((plan.owners, F1 * SUB, 2 * LANES), bf16),
            pltpu.VMEM((plan.owners, F1 * SUB, 2 * LANES), bf16),
            pltpu.VMEM((plan.owners, F1 * SUB, 2 * LANES), f32),
            pltpu.SemaphoreType.DMA((3,)),
            pltpu.SemaphoreType.DMA((sends_needed(plan),)),
            pltpu.SemaphoreType.DMA((2, plan.devices)),
            pltpu.SemaphoreType.DMA((4 * plan.cuts,)),
            pltpu.SemaphoreType.DMA((enders,)),
            pltpu.SemaphoreType.DMA((2,)),
            pltpu.SemaphoreType.DMA((plan.times, plan.owners)),
            pltpu.SemaphoreType.DMA((plan.fine,)),
        ],
        compiler_params=pltpu.CompilerParams(
            collective_id=0,
            has_side_effects=True,
            vmem_limit_bytes=56 * 1024 * 1024,
        ),
    )(s, r, jnp.asarray(waves), jnp.asarray(forward), jnp.asarray(back))


def flipped(index, bit):
    weight = 1 << bit
    return index + weight * (1 - 2 * ((index // weight) % 2))


def flipped_by(index, mask):
    for bit in range(mask.bit_length()):
        if mask >> bit & 1:
            index = flipped(index, bit)
    return index


def order_of(plan):
    bins = F // plan.cuts
    order = np.zeros((plan.fine, 2, SUB, 2, bins), np.float32)
    for fine in range(plan.fine):
        for part in range(2):
            for i in range(plan.per_owner):
                order[fine, part, i, part, plan.fine * i + fine] = 1.0
    return order.reshape(plan.fine * 2 * SUB, 2 * bins).astype(jnp.bfloat16)


def settle_kernel(plan, tiles, order, out):
    rows = plan.fine * 2 * SUB
    wide = lax.dot_general(
        tiles[...].reshape(rows, LANES),
        order[...],
        (((0,), (0,)), ((), ())),
        preferred_element_type=jnp.float32,
    )
    bins = F // plan.cuts
    if plan.lags < LANES:
        pieces = LANES // plan.lags
        which = lax.axis_index("tm") % pieces
        kept = wide[: plan.lags]
        for piece in range(1, pieces):
            kept = jnp.where(
                which == piece, wide[piece * plan.lags : (piece + 1) * plan.lags], kept
            )
        wide = kept
    out[:, 0, :] = wide[:, :bins]
    out[:, 1, :] = wide[:, bins:]


def settled(plan, tiles):
    return pl.pallas_call(
        functools.partial(settle_kernel, plan),
        out_shape=jax.ShapeDtypeStruct((plan.lags, 2, F // plan.cuts), jnp.float32),
        in_specs=[pl.BlockSpec(memory_space=pltpu.VMEM)] * 2,
        out_specs=pl.BlockSpec(memory_space=pltpu.VMEM),
    )(tiles, jnp.asarray(order_of(plan)))


def paired_rows(x):
    samples = x.shape[1] * x.shape[2]
    split = x.reshape(2, samples // LANES, LANES).transpose(1, 0, 2)
    return split.reshape(2 * samples // LANES, LANES)


def on_device(surveillance, reference_signal):
    times, cuts = lax.axis_size("tm"), lax.axis_size("dop")
    samples = surveillance.shape[1] * surveillance.shape[2]
    plan = Plan(times, cuts, samples * times * cuts)
    tiles = dealt_maps(plan, paired_rows(surveillance), paired_rows(reference_signal))
    return settled(plan, tiles)


def solution(mesh):
    return jax.shard_map(
        on_device,
        mesh=mesh,
        in_specs=(P(None, "tm", "dop"), P(None, "tm", "dop")),
        out_specs=P("tm", None, "dop"),
        check_vma=False,
    )
```
